64 devices in a mesh: dp: 4 (over x, y), ep: 16 (over z, core).
Axes of the slice: x: 2, y: 2, z: 8, core: 2. Of those that a mesh axis runs over, the one named last changes fastest.
The devices are a block of a 4x4x8 slice.
Arguments:
- resid_in: bfloat16 [4096, 2560], P(('dp', 'ep')), parts along dimension 0
- expert_ids: int32 [4096, 6], P(('dp', 'ep')), parts along dimension 0
- priority: int32 [4096, 6], P(('dp', 'ep')), parts along dimension 0
- norm_gain: float32 [2560], replicated
- router_w: bfloat16 [2560, 64], replicated
- shared_w1: bfloat16 [2560, 3072], replicated
- shared_w3: bfloat16 [2560, 3072], replicated
- shared_w2: bfloat16 [3072, 2560], replicated
- expert_w1: bfloat16 [64, 2560, 1536], P('ep')
- expert_w3: bfloat16 [64, 2560, 1536], P('ep')
- expert_w2: bfloat16 [64, 1536, 2560], P('ep')
Outputs:
- output: bfloat16 [4096, 2560], P(('dp', 'ep')), parts along dimension 0
There are 4 independent parts. The reference program is written for one: setup_inputs(seed, part) draws one part's arguments, and reference() takes and returns one part's arrays. A program takes and returns all parts, laid end to end along the dimension named above; an argument that names none is the same for every part.
All inputs are finite; a program needn't handle non-finite values.
Results may differ from the reference program's by a relative error of at most 0.00678726.
Values are sent between devices in bfloat16 or wider.
A program may use at most 768 MiB of HBM per device.

```python
import math
import jax
import jax.numpy as jnp
from jax import lax

HIDDEN = 2560
EXPERTS = 64
TOP_K = 6
EXPERT_FF = 1536
SHARED_FF = 3072
GROUPS = 1
TOP_GROUPS = 1
EP_SIZE = 16
TOKENS = 1024
CAPACITY = 384

NORM_EPS = 1e-6
ROUTE_SCALE = 16.0


def draw_routing(route_key):
    key_group, key_score, key_hot, key_prio = jax.random.split(route_key, 4)
    group_width = EXPERTS // GROUPS
    n_cand = TOP_GROUPS * group_width
    local_experts = EXPERTS // EP_SIZE
    hot_range = 1280 * TOP_K // n_cand
    hot_dev = jax.random.permutation(key_hot, EP_SIZE) * hot_range // EP_SIZE
    group_score = jax.random.randint(key_group, (TOKENS, GROUPS), 0, 1 << 20) * GROUPS + jnp.arange(GROUPS)
    group_pick = lax.top_k(group_score, TOP_GROUPS)[1]
    cand_ids = (group_pick[:, :, None] * group_width + jnp.arange(group_width)).reshape(TOKENS, n_cand)
    score_noise = jax.random.randint(key_score, (TOKENS, n_cand), 0, 1024)
    cand_score = (score_noise + hot_dev[cand_ids // local_experts]) * n_cand + jnp.arange(n_cand)
    pick_idx = lax.top_k(cand_score, TOP_K)[1]
    expert_ids = jnp.take_along_axis(cand_ids, pick_idx, axis=1).astype(jnp.int32)
    priority = jax.random.permutation(key_prio, TOKENS * TOP_K).reshape(TOKENS, TOP_K).astype(jnp.int32)
    return expert_ids, priority


def setup_inputs(seed: int = 0, part: int = 0) -> dict:
    root_key = jax.random.key(seed)
    resid_key, route_key = jax.random.split(jax.random.fold_in(root_key, part))
    weight_keys = jax.random.split(jax.random.fold_in(root_key, 1 << 30), 8)
    expert_ids, priority = draw_routing(route_key)
    down_gain = EXPERTS / (10.0 * math.sqrt(TOP_K))
    return dict(
        resid_in=jax.random.normal(resid_key, (TOKENS, HIDDEN), jnp.float32).astype(jnp.bfloat16),
        expert_ids=expert_ids,
        priority=priority,
        norm_gain=1.0 + 0.3 * jax.random.normal(weight_keys[0], (HIDDEN,), jnp.float32),
        router_w=(0.5 * HIDDEN ** -0.5 * jax.random.normal(weight_keys[1], (HIDDEN, EXPERTS), jnp.float32)).astype(jnp.bfloat16),
        shared_w1=(HIDDEN ** -0.5 * jax.random.normal(weight_keys[2], (HIDDEN, SHARED_FF), jnp.float32)).astype(jnp.bfloat16),
        shared_w3=(HIDDEN ** -0.5 * jax.random.normal(weight_keys[3], (HIDDEN, SHARED_FF), jnp.float32)).astype(jnp.bfloat16),
        shared_w2=(SHARED_FF ** -0.5 * jax.random.normal(weight_keys[4], (SHARED_FF, HIDDEN), jnp.float32)).astype(jnp.bfloat16),
        expert_w1=(HIDDEN ** -0.5 * jax.random.normal(weight_keys[5], (EXPERTS, HIDDEN, EXPERT_FF), jnp.float32)).astype(jnp.bfloat16),
        expert_w3=(HIDDEN ** -0.5 * jax.random.normal(weight_keys[6], (EXPERTS, HIDDEN, EXPERT_FF), jnp.float32)).astype(jnp.bfloat16),
        expert_w2=(down_gain * EXPERT_FF ** -0.5 * jax.random.normal(weight_keys[7], (EXPERTS, EXPERT_FF, HIDDEN), jnp.float32)).astype(jnp.bfloat16),
    )


def swiglu_ffn(normed, w_gate, w_up, w_down):
    up_a = jnp.dot(normed, w_gate, preferred_element_type=jnp.float32)
    up_b = jnp.dot(normed, w_up, preferred_element_type=jnp.float32)
    hidden_act = (jax.nn.silu(up_a) * up_b).astype(jnp.bfloat16)
    return jnp.dot(hidden_act, w_down, preferred_element_type=jnp.float32).astype(jnp.bfloat16)


def keep_mask(expert_ids, priority):
    n_assign = TOKENS * TOP_K
    owners = (expert_ids // (EXPERTS // EP_SIZE)).reshape(n_assign)
    prio_flat = priority.reshape(n_assign)
    owner_by_rank = jnp.zeros((n_assign,), jnp.int32).at[prio_flat].set(owners)
    dest_hits = (owner_by_rank[:, None] == jnp.arange(EP_SIZE, dtype=jnp.int32)).astype(jnp.int32)
    before = jnp.cumsum(dest_hits, axis=0) - dest_hits
    rank_by_prio = jnp.sum(before * dest_hits, axis=1)
    return (rank_by_prio[prio_flat] < CAPACITY).reshape(TOKENS, TOP_K)


def routed_sum(normed, expert_ids, flat_gates, expert_w1, expert_w3, expert_w2):
    n_assign = TOKENS * TOP_K
    row_block = max(8, n_assign // (32 * EXPERTS) * 8)
    n_blocks = n_assign // row_block + EXPERTS + 1
    flat_ids = expert_ids.reshape(n_assign)
    sort_order = jnp.argsort(flat_ids * n_assign + jnp.arange(n_assign, dtype=jnp.int32)).astype(jnp.int32)
    counts = jax.ops.segment_sum(jnp.ones((n_assign,), jnp.int32), flat_ids, num_segments=EXPERTS)
    padded = (counts + row_block - 1) // row_block * row_block
    pad_start = jnp.cumsum(padded) - padded
    sort_start = jnp.cumsum(counts) - counts
    sorted_ids = flat_ids[sort_order]
    dest_row = pad_start[sorted_ids] + jnp.arange(n_assign, dtype=jnp.int32) - sort_start[sorted_ids]
    row_src = jnp.full((n_blocks * row_block,), n_assign, jnp.int32).at[dest_row].set(sort_order)
    block_first = jnp.arange(n_blocks, dtype=jnp.int32) * row_block
    block_expert = jnp.sum((pad_start[None, :] <= block_first[:, None]).astype(jnp.int32), axis=1) - 1
    normed_pad = jnp.concatenate([normed, jnp.zeros((1, HIDDEN), normed.dtype)], axis=0)
    gates_pad = jnp.concatenate([flat_gates, jnp.zeros((1,), flat_gates.dtype)])

    def one_block(routed_acc, block_args):
        src_rows, expert = block_args
        tok_rows = src_rows // TOP_K
        expert_out = swiglu_ffn(normed_pad[tok_rows], expert_w1[expert], expert_w3[expert], expert_w2[expert])
        weighted = expert_out.astype(jnp.float32) * gates_pad[src_rows][:, None]
        return routed_acc.at[tok_rows].add(weighted), None

    routed_acc = lax.scan(one_block, jnp.zeros((TOKENS + 1, HIDDEN), jnp.float32), (row_src.reshape(n_blocks, row_block), block_expert))[0]
    return routed_acc[:TOKENS]


def reference(resid_in, expert_ids, priority, norm_gain, router_w, shared_w1, shared_w3, shared_w2, expert_w1, expert_w3, expert_w2):
    resid32 = resid_in.astype(jnp.float32)
    inv_rms = lax.rsqrt(jnp.mean(resid32 * resid32, axis=1, keepdims=True) + NORM_EPS)
    normed = (resid32 * inv_rms * norm_gain).astype(jnp.bfloat16)
    gate_probs = jax.nn.softmax(jnp.dot(normed, router_w, preferred_element_type=jnp.float32), axis=1)
    gate_vals = ROUTE_SCALE * jnp.take_along_axis(gate_probs, expert_ids, axis=1)
    kept_mask = keep_mask(expert_ids, priority)
    flat_gates = jnp.where(kept_mask, gate_vals, 0.0).reshape(TOKENS * TOP_K)
    shared_out = swiglu_ffn(normed, shared_w1, shared_w3, shared_w2)
    routed = routed_sum(normed, expert_ids, flat_gates, expert_w1, expert_w3, expert_w2)
    return (resid32 + shared_out.astype(jnp.float32) + routed).astype(jnp.bfloat16)
```

```python
import functools

import jax
import jax.numpy as jnp
from jax import lax
from jax.experimental import pallas as pl
from jax.experimental.pallas import tpu as pltpu
from jax.sharding import PartitionSpec as P

NORM_EPS = 1e-6
ROUTE_SCALE = 16.0
KC = 256
TILE = 128
KPAD = 8
F32 = jnp.float32
BF16 = jnp.bfloat16


def dot(a, b):
    return jnp.dot(a, b, preferred_element_type=F32)


def ring_place(dm):
    n = dm.n_chip
    me = lax.axis_index("ep")
    chip = me // 2
    core = me - 2 * chip
    d = 1 - 2 * core

    def at(h):
        return lax.rem(chip + h * d + 2 * n, n)

    return me, chip, core, at, 2 * chip + 1 - core, 2 * at(1) + core, 2 * at(-1) + core


def rcopy(src, dst, ssem, rsem, dev):
    return pltpu.make_async_remote_copy(src_ref=src, dst_ref=dst, send_sem=ssem, recv_sem=rsem,
                                        device_id={"ep": dev}, device_id_type=pl.DeviceIdType.MESH)


def entry_barrier(devs):
    barrier = pltpu.get_barrier_semaphore()
    for dev in devs:
        pl.semaphore_signal(barrier, inc=1, device_id={"ep": dev}, device_id_type=pl.DeviceIdType.MESH)
    pl.semaphore_wait(barrier, len(devs))


def cond(static, pred, fn):
    if static:
        if pred:
            fn()
    else:
        pl.when(pred)(fn)


def start(copies):
    for c in copies:
        c.start()


def wait(copies):
    for c in copies:
        c.wait()


def gather_kernel(dm, b_ref, info_ref, X, PG, WC, TE,
                  I, SLT, GLT, lsem, xs_ring, xr_ring, xs_d2d, xr_d2d, is_ring, ir_ring, is_d2d, ir_d2d, p_s, p_r):
    n = dm.n_chip
    hops = n // 2
    tok = dm.tok
    crows = 2 * tok
    nj = dm.nj
    off = hops + 1
    slots = dm.slots
    n_tiles = slots // TILE
    group = n * crows
    me, chip, core, at, partner, down, up = ring_place(dm)
    half = pl.ds(pl.multiple_of(core * tok, tok), tok)
    entry_barrier((partner, down, up))

    own_x = X.at[:, chip, half, :]
    own_i = I.at[chip, core]
    first = [rcopy(b_ref, own_x, p_s.at[0], p_r.at[0], partner), rcopy(info_ref, own_i, p_s.at[1], p_r.at[1], partner)]
    start(first)
    local = [pltpu.make_async_copy(b_ref, own_x, lsem.at[0]), pltpu.make_async_copy(info_ref, own_i, lsem.at[1])]
    start(local)
    wait(local)
    for c in first:
        c.wait_recv()

    def x_block(j, h, rows_half):
        return X.at[j, at(-h), half, :] if rows_half else X.at[j, at(-h)]

    def x_ring(j, h):
        blk = x_block(j, h, h + 1 == hops)
        return rcopy(blk, blk, xs_ring.at[h, j], xr_ring.at[h, j], down)

    def x_ring_in(j, h):
        blk = x_block(j, h, h == hops)
        return rcopy(blk, blk, xs_ring.at[h - 1, j], xr_ring.at[h - 1, j], down)

    def x_d2d(j, h):
        blk = x_block(j, h, h == hops)
        return rcopy(blk, blk, xs_d2d.at[h - 1, j], xr_d2d.at[h - 1, j], partner)

    def x_d2d_in(j, h):
        blk = X.at[j, at(h), pl.ds(pl.multiple_of((1 - core) * tok, tok), tok), :] if h == hops else X.at[j, at(h)]
        return rcopy(blk, blk, xs_d2d.at[h - 1, j], xr_d2d.at[h - 1, j], partner)

    def comm(s, static):
        def hop(h):
            j = s - h

            def run():
                if h > 0:
                    x_ring_in(j, h).wait_recv()
                if h < hops:
                    x_ring(j, h).start()
                if h > 0:
                    x_d2d(j, h).start()
            cond(static, (j < nj and j >= 0) if static else (j < nj), run)
        hop(0)
        for h in range(hops, 0, -1):
            hop(h)

    def i_block(h, rows_half, sign=-1, c=None):
        return I.at[at(sign * h), core if c is None else c] if rows_half else I.at[at(sign * h)]

    def comm_info(h):
        if h > 0:
            blk = i_block(h, h == hops)
            rcopy(blk, blk, is_ring.at[h - 1], ir_ring.at[h - 1], down).wait_recv()
        if h < hops:
            blk = i_block(h, h + 1 == hops)
            rcopy(blk, blk, is_ring.at[h], ir_ring.at[h], down).start()
        if h > 0:
            blk = i_block(h, h == hops)
            rcopy(blk, blk, is_d2d.at[h - 1], ir_d2d.at[h - 1], partner).start()

    for s in range(off):
        comm_info(s)
        comm(s, True)

    for h in range(1, hops + 1):
        blk = i_block(h, h == hops, 1, 1 - core)
        rcopy(blk, blk, is_d2d.at[h - 1], ir_d2d.at[h - 1], partner).wait_recv()

    lanes = crows
    nr = n * KPAD

    def field(i):
        rows = pl.ds(i * KPAD, KPAD)
        return (I[:, 0, rows, :] + I[:, 1, rows, :]).reshape(nr, lanes)

    mine_e = field(0) - (me * dm.local_e).astype(F32)
    prio = field(1)
    gate = field(2)
    mine = (mine_e >= 0) & (mine_e < dm.local_e)
    key = jnp.where(mine, prio, 1e9)
    cut = jnp.zeros((1, 1), F32)
    bit = 1 << (group * dm.top_k).bit_length()
    while bit >= 1:
        cand = cut + float(bit)
        cnt = jnp.sum(jnp.where(key < cand, 1.0, 0.0), keepdims=True)
        cut = jnp.where(cnt <= float(dm.capacity), cand, cut)
        bit //= 2
    kept = key < cut
    masks = [jnp.where(kept & (mine_e == float(e)), 1.0, 0.0) for e in range(dm.local_e)]
    stack = jnp.concatenate(masks, axis=0)
    li = lax.broadcasted_iota(jnp.int32, (lanes, lanes), 0)
    lj = lax.broadcasted_iota(jnp.int32, (lanes, lanes), 1)
    upper = jnp.where(li <= lj, 1.0, 0.0).astype(BF16)
    inrow = dot(stack.astype(BF16), upper)
    total_rows = dm.local_e * nr
    rowtot = jnp.broadcast_to(inrow[:, lanes - 1:lanes], (total_rows, lanes))
    ri = lax.broadcasted_iota(jnp.int32, (total_rows, total_rows), 0)
    rj = lax.broadcasted_iota(jnp.int32, (total_rows, total_rows), 1)
    lower = jnp.where((ri > rj) & (ri // nr == rj // nr), 1.0, 0.0).astype(BF16)
    before = dot(lower, rowtot.astype(BF16))
    slot_of = jnp.full((nr, lanes), -1.0, F32)
    base = jnp.zeros((1, lanes), F32)
    bound = jnp.int32(0)
    bounds = []
    for e in range(dm.local_e):
        rows = slice(e * nr, (e + 1) * nr)
        pos = base + before[rows] + inrow[rows] - 1.0
        slot_of = jnp.where(masks[e] > 0.5, pos, slot_of)
        last = (e + 1) * nr - 1
        count = before[last:last + 1] + rowtot[last:last + 1]
        base = base + jnp.floor((count + (TILE - 1.0)) * (1.0 / TILE)) * TILE
        count_i = jnp.sum(jnp.where(kept & (mine_e == float(e)), 1, 0))
        bound = bound + (count_i + (TILE - 1)) // TILE
        bounds.append(bound)
    tile_e = [sum(jnp.where(bounds[e] <= i, 1, 0) for e in range(dm.local_e - 1)) for i in range(n_tiles)]

    slot_t = slot_of.T
    gate_t = gate.T
    for c in range(n):
        SLT[c] = slot_t[:, c * KPAD:(c + 1) * KPAD]
        GLT[c] = gate_t[:, c * KPAD:(c + 1) * KPAD]
        for r in range(n_tiles):
            srow = (lax.broadcasted_iota(jnp.int32, (TILE, lanes), 0) + r * TILE).astype(F32)
            hit = jnp.zeros((TILE, lanes), F32)
            for k in range(dm.top_k):
                hit = jnp.where(slot_of[c * KPAD + k:c * KPAD + k + 1] == srow, 1.0, hit)
            PG[pl.ds(r * TILE, TILE), pl.ds(c * lanes, lanes)] = hit.astype(BF16)

    for i in range(n_tiles):
        TE[i] = tile_e[i]

    def combine_rows(c):
        sl = SLT[c]
        gl = GLT[c]
        rows = pl.ds(pl.multiple_of(c * crows, crows), crows)
        for p in range(slots // KC):
            scol = (lax.broadcasted_iota(jnp.int32, (crows, KC), 1) + p * KC).astype(F32)
            w = jnp.zeros((crows, KC), F32)
            for k in range(dm.top_k):
                w = jnp.where(sl[:, k:k + 1] == scol, gl[:, k:k + 1], w)
            for i in range(3):
                part = w.astype(BF16)
                WC[rows, pl.ds(i * slots + p * KC, KC)] = part
                w = w - part.astype(F32)

    def step(j, carry):
        comm(j + off, False)

        @pl.when(j < n)
        def _():
            combine_rows(j)
        return carry

    lax.fori_loop(0, nj - 1, step, 0)
    for c in range(nj - 1, n):
        combine_rows(c)

    def arrive(j, carry):
        for h in range(1, hops + 1):
            x_d2d_in(j, h).wait_recv()
        return carry

    lax.fori_loop(0, nj, arrive, 0)
    for c in first:
        c.wait_send()
    for h in range(hops):
        blk = i_block(h, h + 1 == hops)
        rcopy(blk, blk, is_ring.at[h], ir_ring.at[h], down).wait_send()
        blk = i_block(h + 1, h + 1 == hops)
        rcopy(blk, blk, is_d2d.at[h], ir_d2d.at[h], partner).wait_send()

    def drain(j, carry):
        for h in range(hops):
            x_ring(j, h).wait_send()
            x_d2d(j, h + 1).wait_send()
        return carry

    lax.fori_loop(0, nj, drain, 0)


def up_kernel(dm, te_ref, x_ref, pg_ref, w1_ref, w3_ref, h_ref, acc_ref):
    nt = dm.ff // KC
    j = pl.program_id(0)

    @pl.when(j == 0)
    def _():
        acc_ref[...] = jnp.zeros(acc_ref.shape, F32)

    xg = dot(pg_ref[...], x_ref[0].reshape(pg_ref.shape[1], KC)).astype(BF16)
    for i in range(dm.slots // TILE):
        xi = xg[i * TILE:(i + 1) * TILE]
        for m, w_ref in enumerate((w1_ref, w3_ref)):
            for c in range(nt):
                rows = pl.ds((m * nt + c) * dm.slots + i * TILE, TILE)
                acc_ref[rows, :] += dot(xi, w_ref[te_ref[i], :, pl.ds(c * KC, KC)])

    @pl.when(j == pl.num_programs(0) - 1)
    def _():
        for i in range(dm.slots // TILE):
            for c in range(nt):
                a = acc_ref[pl.ds(c * dm.slots + i * TILE, TILE), :]
                g = acc_ref[pl.ds((nt + c) * dm.slots + i * TILE, TILE), :]
                h_ref[pl.ds(i * TILE, TILE), pl.ds(c * KC, KC)] = (jax.nn.silu(a) * g).astype(BF16)


def down_kernel(dm, H, WC, TE, shared_ref, resid_ref, ew2, out_ref,
                BIG, V2A, V2B, E3, PR, RR, FR, vsem, qs, qr, rs, rr, fs, fr):
    n = dm.n_chip
    hops = n // 2
    tok = dm.tok
    crows = 2 * tok
    nj = dm.nj
    slots = dm.slots
    n_tiles = slots // TILE
    group = n * crows
    me, chip, core, at, partner, down, up = ring_place(dm)
    V2 = (V2A, V2B)

    def down_copies(j, slot):
        cols = pl.ds(pl.multiple_of(j * KC, KC), KC)
        return [pltpu.make_async_copy(ew2.at[:, :, cols], V2[slot], vsem.at[slot])]

    start(down_copies(0, 0))
    start(down_copies(1, 1))
    entry_barrier((partner, down, up))

    pr_off = [448, 0, 128, 256, 384]
    assert crows == 128 and hops == 4

    def dblk(j, dest, row, size):
        return pl.ds(pl.multiple_of(j * group + dest * crows + row, tok), size)

    def q_copy(j, h):
        if h == 0:
            src, size = BIG.at[dblk(j, chip, (1 - core) * tok, tok), :], tok
        elif h == hops:
            src, size = BIG.at[dblk(j, at(-h), (1 - core) * tok, tok), :], tok
        else:
            src, size = BIG.at[dblk(j, at(-h), 0, crows), :], crows
        return rcopy(src, PR.at[j, pl.ds(pr_off[h], size), :], qs.at[h, j], qr.at[h, j], partner)

    rr_off = [0, 64, 192, 320]

    def r_copy(j, g):
        h = hops - g
        src, size = (BIG.at[dblk(j, at(h), core * tok, tok), :], tok) if g == 0 else (BIG.at[dblk(j, at(h), 0, crows), :], crows)
        return rcopy(src, RR.at[j, pl.ds(rr_off[g], size), :], rs.at[g, j], rr.at[g, j], down)

    def f_copy(j):
        return rcopy(RR.at[j, pl.ds(pl.multiple_of(rr_off[hops - 1] + (1 - core) * tok, tok), tok), :], FR.at[j], fs.at[j], fr.at[j], partner)

    def finish(j):
        q_copy(j, 0).wait_recv()
        f_copy(j).wait_recv()
        cols = pl.ds(pl.multiple_of(j * KC, KC), KC)
        routed = BIG[dblk(j, chip, core * tok, tok), :] + PR[j, pl.ds(pr_off[0], tok), :]
        routed = routed + RR[j, pl.ds(pl.multiple_of(rr_off[hops - 1] + core * tok, tok), tok), :] + FR[j]
        out_ref[:, cols] = (resid_ref[:, cols].astype(F32) + shared_ref[:, cols].astype(F32) + routed).astype(BF16)

    def turn(j):
        r_copy(j, hops - 1).wait_recv()
        f_copy(j).start()

    def relay(j, g):
        h = hops - g
        q_copy(j, h).wait_recv()
        if g == 0:
            rows = dblk(j, at(h), core * tok, tok)
            BIG[rows, :] += PR[j, pl.ds(pr_off[h], tok), :]
        else:
            r_copy(j, g - 1).wait_recv()
            rows = dblk(j, at(h), 0, crows)
            if g == 1:
                BIG[rows, :] += PR[j, pl.ds(pr_off[h], crows), :]
                hrows = dblk(j, at(h), core * tok, tok)
                BIG[hrows, :] += RR[j, pl.ds(rr_off[0], tok), :]
            else:
                BIG[rows, :] += PR[j, pl.ds(pr_off[h], crows), :] + RR[j, pl.ds(rr_off[g - 1], crows), :]
        r_copy(j, g).start()

    def ring(s, static):
        def ok(j):
            return (0 <= j < nj) if static else (j >= 0)
        cond(static, ok(s - hops - 2), lambda: finish(s - hops - 2))
        cond(static, ok(s - hops - 1), lambda: turn(s - hops - 1))
        for g in range(hops - 1, -1, -1):
            cond(static, ok(s - 1 - g), functools.partial(relay, s - 1 - g, g))

    def down_step(j, slot):
        ring(j, False)
        wait(down_copies(j, slot))
        for i in range(n_tiles):
            e = dot(H[pl.ds(i * TILE, TILE), :], V2[slot][TE[i]]).astype(BF16)
            for p in range(3):
                E3[pl.ds(p * slots + i * TILE, TILE), :] = e
        for r in range(group // KC):
            rows = pl.ds(pl.multiple_of(j * group + r * KC, KC), KC)
            BIG[rows, :] = dot(WC[pl.ds(r * KC, KC), :], E3[...])
        for h in range(hops, -1, -1):
            q_copy(j, h).start()

        @pl.when(j + 2 < nj)
        def _():
            start(down_copies(j + 2, slot))

    def down_pair(p, carry):
        for q in range(2):
            down_step(2 * p + q, q)
        return carry

    lax.fori_loop(0, nj // 2, down_pair, 0)
    for s in range(nj, nj + hops + 2):
        ring(s, True)

    def drain(j, carry):
        for h in range(hops):
            r_copy(j, h).wait_send()
        for h in range(hops + 1):
            q_copy(j, h).wait_send()
        f_copy(j).wait_send()
        return carry

    lax.fori_loop(0, nj, drain, 0)


class Dims:
    pass


def solution(mesh):
    n_ep = mesh.shape['ep']
    tok_spec = P(('dp', 'ep'))
    expert_spec = P('ep')

    def device_fn(resid_in, expert_ids, priority, norm_gain, router_w, shared_w1, shared_w3, shared_w2, expert_w1, expert_w3, expert_w2):
        dm = Dims()
        dm.n_chip = n_ep // 2
        dm.tok, dm.hidden = resid_in.shape
        dm.top_k = expert_ids.shape[1]
        dm.local_e = expert_w1.shape[0]
        dm.ff = expert_w1.shape[2]
        dm.capacity = dm.tok * dm.top_k
        dm.nj = dm.hidden // KC
        dm.slots = (dm.capacity + dm.local_e * (TILE - 1)) // TILE * TILE
        hops = dm.n_chip // 2
        assert dm.nj % 2 == 0
        nj, tok, ff, slots = dm.nj, dm.tok, dm.ff, dm.slots
        group = dm.n_chip * 2 * tok

        resid32 = resid_in.astype(F32)
        inv_rms = lax.rsqrt(jnp.mean(resid32 * resid32, axis=1, keepdims=True) + NORM_EPS)
        normed = (resid32 * inv_rms * norm_gain).astype(BF16)
        probs = jax.nn.softmax(jnp.dot(normed, router_w, preferred_element_type=F32), axis=1)
        pick = expert_ids[:, :, None] == jnp.arange(router_w.shape[1], dtype=jnp.int32)
        gates = ROUTE_SCALE * jnp.sum(jnp.where(pick, probs[:, None, :], 0.0), axis=2)
        blocks = normed.reshape(tok, nj, KC).transpose(1, 0, 2)
        shared_act = (jax.nn.silu(dot(normed, shared_w1)) * dot(normed, shared_w3)).astype(BF16)
        shared_out = dot(shared_act, shared_w2).astype(BF16)

        def field(a, fill):
            return jnp.pad(a.astype(F32).T, ((0, KPAD - dm.top_k), (0, 0)), constant_values=fill)

        part = jnp.concatenate([field(expert_ids, -1.0), field(priority, 0.0), field(gates, 0.0)], axis=0)
        core = lax.axis_index('ep') % 2
        info = jnp.concatenate([jnp.where(core == 0, part, 0.0), jnp.where(core == 0, 0.0, part)], axis=1)

        vm = pl.BlockSpec(memory_space=pltpu.VMEM)
        sm = pl.BlockSpec(memory_space=pltpu.SMEM)
        hbm = pl.BlockSpec(memory_space=pl.ANY)
        dma = pltpu.SemaphoreType.DMA
        le = dm.local_e
        rows_all, pick_rows, mix, tile_e = pl.pallas_call(
            functools.partial(gather_kernel, dm),
            out_shape=(jax.ShapeDtypeStruct((nj, dm.n_chip, 2 * tok, KC), BF16), jax.ShapeDtypeStruct((slots, group), BF16),
                       jax.ShapeDtypeStruct((group, 3 * slots), BF16), jax.ShapeDtypeStruct((slots // TILE,), jnp.int32)),
            in_specs=[vm, vm],
            out_specs=(vm, vm, vm, sm),
            scratch_shapes=[
                pltpu.VMEM((dm.n_chip, 2, 3 * KPAD, 2 * tok), F32),
                pltpu.VMEM((dm.n_chip, 2 * tok, KPAD), F32),
                pltpu.VMEM((dm.n_chip, 2 * tok, KPAD), F32),
                dma((2,)),
                dma((hops, nj)), dma((hops, nj)), dma((hops, nj)), dma((hops, nj)),
                dma((hops,)), dma((hops,)), dma((hops,)), dma((hops,)), dma((2,)), dma((2,)),
            ],
            compiler_params=pltpu.CompilerParams(collective_id=0, has_side_effects=True, vmem_limit_bytes=24 << 20),
        )(blocks, info)
        h_act = pl.pallas_call(
            functools.partial(up_kernel, dm),
            out_shape=jax.ShapeDtypeStruct((slots, ff), BF16),
            grid=(nj,),
            in_specs=[sm, pl.BlockSpec((1, dm.n_chip, 2 * tok, KC), lambda j: (j, 0, 0, 0)), vm,
                      pl.BlockSpec((le, KC, ff), lambda j: (0, j, 0)), pl.BlockSpec((le, KC, ff), lambda j: (0, j, 0))],
            out_specs=vm,
            scratch_shapes=[pltpu.VMEM((2 * (ff // KC) * slots, KC), F32)],
            compiler_params=pltpu.CompilerParams(vmem_limit_bytes=40 << 20),
        )(tile_e, rows_all, pick_rows, expert_w1, expert_w3)
        return pl.pallas_call(
            functools.partial(down_kernel, dm),
            out_shape=jax.ShapeDtypeStruct((tok, dm.hidden), BF16),
            in_specs=[vm, vm, sm, vm, vm, hbm],
            out_specs=vm,
            scratch_shapes=[
                pltpu.VMEM((nj * group, KC), F32),
                pltpu.VMEM((le, ff, KC), BF16),
                pltpu.VMEM((le, ff, KC), BF16),
                pltpu.VMEM((3 * slots, KC), BF16),
                pltpu.VMEM((nj, 8 * tok, KC), F32),
                pltpu.VMEM((nj, 7 * tok, KC), F32),
                pltpu.VMEM((nj, tok, KC), F32),
                dma((2,)),
                dma((hops + 1, nj)), dma((hops + 1, nj)), dma((hops, nj)), dma((hops, nj)), dma((nj,)), dma((nj,)),
            ],
            compiler_params=pltpu.CompilerParams(collective_id=1, has_side_effects=True, vmem_limit_bytes=48 << 20),
        )(h_act, mix, tile_e, shared_out, resid_in, expert_w2)

    return jax.shard_map(device_fn, mesh=mesh, in_specs=(tok_spec, tok_spec, tok_spec, P(), P(), P(), P(), P(), expert_spec, expert_spec, expert_spec), out_specs=tok_spec, check_vma=False)
```

```python
import functools

import jax
import jax.numpy as jnp
from jax import lax
from jax.experimental import pallas as pl
from jax.experimental.pallas import tpu as pltpu
from jax.sharding import PartitionSpec as P

NORM_EPS = 1e-6
ROUTE_SCALE = 16.0
KC = 256
TILE = 128
KPAD = 8
F32 = jnp.float32
BF16 = jnp.bfloat16


def dot(a, b):
    return jnp.dot(a, b, preferred_element_type=F32)


def ring_place(dm):
    n = dm.n_chip
    me = lax.axis_index("ep")
    chip = me // 2
    core = me - 2 * chip
    d = 1 - 2 * core

    def at(h):
        return lax.rem(chip + h * d + 2 * n, n)

    return me, chip, core, at, 2 * chip + 1 - core, 2 * at(1) + core, 2 * at(-1) + core


def rcopy(src, dst, ssem, rsem, dev):
    return pltpu.make_async_remote_copy(src_ref=src, dst_ref=dst, send_sem=ssem, recv_sem=rsem,
                                        device_id={"ep": dev}, device_id_type=pl.DeviceIdType.MESH)


def entry_barrier(devs):
    barrier = pltpu.get_barrier_semaphore()
    for dev in devs:
        pl.semaphore_signal(barrier, inc=1, device_id={"ep": dev}, device_id_type=pl.DeviceIdType.MESH)
    pl.semaphore_wait(barrier, len(devs))


def cond(static, pred, fn):
    if static:
        if pred:
            fn()
    else:
        pl.when(pred)(fn)


def start(copies):
    for c in copies:
        c.start()


def wait(copies):
    for c in copies:
        c.wait()


def gather_kernel(dm, b_ref, info_ref, sw1, sw3, X, PG, WC, HS, TE,
                  I, SLT, GLT, SACC, WS, lsem, wsem, xs_ring, xr_ring, xs_d2d, xr_d2d, is_ring, ir_ring, is_d2d, ir_d2d, p_s, p_r):
    n = dm.n_chip
    hops = n // 2
    tok = dm.tok
    crows = 2 * tok
    nj = dm.nj
    slots = dm.slots
    n_tiles = slots // TILE
    group = n * crows
    me, chip, core, at, partner, down, up = ring_place(dm)
    half = pl.ds(pl.multiple_of(core * tok, tok), tok)
    sff = dm.sff

    def shared_copies(t):
        rows = pl.ds(t * KC, KC)
        return [pltpu.make_async_copy(src.at[rows, :], WS.at[t % 3, m], wsem.at[t % 3, m]) for m, src in enumerate((sw1, sw3))]

    def shared_stage(t):
        wait(shared_copies(t))
        x = b_ref[t]
        for m in range(2):
            for c in range(sff // KC):
                dst = pl.ds(m * sff + c * KC, KC)
                val = dot(x, WS[t % 3, m, :, pl.ds(c * KC, KC)])
                if t == 0:
                    SACC[:, dst] = val
                else:
                    SACC[:, dst] += val
        if t + 3 < nj:
            start(shared_copies(t + 3))

    for t in range(3):
        start(shared_copies(t))
    entry_barrier((partner, down, up))

    own_x = X.at[:, chip, half, :]
    own_i = I.at[chip, core]
    first = [rcopy(b_ref, own_x, p_s.at[0], p_r.at[0], partner), rcopy(info_ref, own_i, p_s.at[1], p_r.at[1], partner)]
    start(first)
    local = [pltpu.make_async_copy(b_ref, own_x, lsem.at[0]), pltpu.make_async_copy(info_ref, own_i, lsem.at[1])]
    start(local)
    wait(local)
    for c in first:
        c.wait_recv()

    def x_block(j, h, rows_half):
        return X.at[j, at(-h), half, :] if rows_half else X.at[j, at(-h)]

    def x_ring(j, h):
        blk = x_block(j, h, h + 1 == hops)
        return rcopy(blk, blk, xs_ring.at[h, j], xr_ring.at[h, j], down)

    def x_ring_in(j, h):
        blk = x_block(j, h, h == hops)
        return rcopy(blk, blk, xs_ring.at[h - 1, j], xr_ring.at[h - 1, j], down)

    def x_d2d(j, h):
        blk = x_block(j, h, h == hops)
        return rcopy(blk, blk, xs_d2d.at[h - 1, j], xr_d2d.at[h - 1, j], partner)

    def x_d2d_in(j, h):
        blk = X.at[j, at(h), pl.ds(pl.multiple_of((1 - core) * tok, tok), tok), :] if h == hops else X.at[j, at(h)]
        return rcopy(blk, blk, xs_d2d.at[h - 1, j], xr_d2d.at[h - 1, j], partner)

    def forward(h, j):
        if h > 0:
            x_ring_in(j, h).wait_recv()
        if h < hops:
            x_ring(j, h).start()
        if h > 0:
            x_d2d(j, h).start()

    def i_block(h, rows_half, sign=-1, c=None):
        return I.at[at(sign * h), core if c is None else c] if rows_half else I.at[at(sign * h)]

    def comm_info(h):
        if h > 0:
            blk = i_block(h, h == hops)
            rcopy(blk, blk, is_ring.at[h - 1], ir_ring.at[h - 1], down).wait_recv()
        if h < hops:
            blk = i_block(h, h + 1 == hops)
            rcopy(blk, blk, is_ring.at[h], ir_ring.at[h], down).start()
        if h > 0:
            blk = i_block(h, h == hops)
            rcopy(blk, blk, is_d2d.at[h - 1], ir_d2d.at[h - 1], partner).start()

    per = (nj + hops - 1) // hops
    for h in range(hops):
        comm_info(h)
        for j in range(h * per, min((h + 1) * per, nj)):
            forward(0, j)
    for j in range(nj // 2 + 1):
        forward(1, j)
    comm_info(hops)
    shared_stage(0)

    for h in range(1, hops + 1):
        blk = i_block(h, h == hops, 1, 1 - core)
        rcopy(blk, blk, is_d2d.at[h - 1], ir_d2d.at[h - 1], partner).wait_recv()

    lanes = crows
    nr = n * KPAD

    def field(i):
        rows = pl.ds(i * KPAD, KPAD)
        return (I[:, 0, rows, :] + I[:, 1, rows, :]).reshape(nr, lanes)

    mine_e = field(0) - (me * dm.local_e).astype(F32)
    prio = field(1)
    gate = field(2)
    mine = (mine_e >= 0) & (mine_e < dm.local_e)
    key = jnp.where(mine, prio, 1e9)
    cut = jnp.zeros((1, 1), F32)
    bit = 1 << (group * dm.top_k).bit_length()
    while bit >= 1:
        cand = cut + float(bit)
        cnt = jnp.sum(jnp.where(key < cand, 1.0, 0.0), keepdims=True)
        cut = jnp.where(cnt <= float(dm.capacity), cand, cut)
        bit //= 2
    kept = key < cut
    masks = [jnp.where(kept & (mine_e == float(e)), 1.0, 0.0) for e in range(dm.local_e)]
    stack = jnp.concatenate(masks, axis=0)
    li = lax.broadcasted_iota(jnp.int32, (lanes, lanes), 0)
    lj = lax.broadcasted_iota(jnp.int32, (lanes, lanes), 1)
    upper = jnp.where(li <= lj, 1.0, 0.0).astype(BF16)
    inrow = dot(stack.astype(BF16), upper)
    total_rows = dm.local_e * nr
    rowtot = jnp.broadcast_to(inrow[:, lanes - 1:lanes], (total_rows, lanes))
    ri = lax.broadcasted_iota(jnp.int32, (total_rows, total_rows), 0)
    rj = lax.broadcasted_iota(jnp.int32, (total_rows, total_rows), 1)
    lower = jnp.where((ri > rj) & (ri // nr == rj // nr), 1.0, 0.0).astype(BF16)
    before = dot(lower, rowtot.astype(BF16))
    slot_of = jnp.full((nr, lanes), -1.0, F32)
    base = jnp.zeros((1, lanes), F32)
    bound = jnp.int32(0)
    bounds = []
    for e in range(dm.local_e):
        rows = slice(e * nr, (e + 1) * nr)
        pos = base + before[rows] + inrow[rows] - 1.0
        slot_of = jnp.where(masks[e] > 0.5, pos, slot_of)
        last = (e + 1) * nr - 1
        count = before[last:last + 1] + rowtot[last:last + 1]
        base = base + jnp.floor((count + (TILE - 1.0)) * (1.0 / TILE)) * TILE
        count_i = jnp.sum(jnp.where(kept & (mine_e == float(e)), 1, 0))
        bound = bound + (count_i + (TILE - 1)) // TILE
        bounds.append(bound)
    tile_e = [sum(jnp.where(bounds[e] <= i, 1, 0) for e in range(dm.local_e - 1)) for i in range(n_tiles)]

    slot_t = slot_of.T
    gate_t = gate.T
    for c in range(n):
        SLT[c] = slot_t[:, c * KPAD:(c + 1) * KPAD]
        GLT[c] = gate_t[:, c * KPAD:(c + 1) * KPAD]
        for r in range(n_tiles):
            srow = (lax.broadcasted_iota(jnp.int32, (TILE, lanes), 0) + r * TILE).astype(F32)
            hit = jnp.zeros((TILE, lanes), F32)
            for k in range(dm.top_k):
                hit = jnp.where(slot_of[c * KPAD + k:c * KPAD + k + 1] == srow, 1.0, hit)
            PG[pl.ds(r * TILE, TILE), pl.ds(c * lanes, lanes)] = hit.astype(BF16)

    for i in range(n_tiles):
        TE[i] = tile_e[i]

    def combine_rows(c):
        sl = SLT[c]
        gl = GLT[c]
        rows = pl.ds(c * crows, crows)
        for p in range(slots // KC):
            scol = (lax.broadcasted_iota(jnp.int32, (crows, KC), 1) + p * KC).astype(F32)
            w = jnp.zeros((crows, KC), F32)
            for k in range(dm.top_k):
                w = jnp.where(sl[:, k:k + 1] == scol, gl[:, k:k + 1], w)
            for i in range(3):
                part = w.astype(BF16)
                WC[rows, pl.ds(i * slots + p * KC, KC)] = part
                w = w - part.astype(F32)

    todo = [(1, j) for j in range(nj // 2 + 1, nj)] + [(h, j) for h in range(2, hops + 1) for j in range(nj)]
    work = []
    for t in range(1, nj):
        work.append(functools.partial(shared_stage, t))
        if t - 1 < n:
            work.append(functools.partial(combine_rows, t - 1))
    last = len(todo) - nj
    for u, (h, j) in enumerate(todo):
        forward(h, j)
        while work and len(work) > (2 * nj - 2) * (last - 1 - u) // last:
            work.pop(0)()
    for w in work:
        w()
    for c in range(sff // KC):
        a = SACC[:, pl.ds(c * KC, KC)]
        g = SACC[:, pl.ds(sff + c * KC, KC)]
        HS[:, pl.ds(c * KC, KC)] = (jax.nn.silu(a) * g).astype(BF16)

    def arrive(j, carry):
        for h in range(1, hops + 1):
            x_d2d_in(j, h).wait_recv()
        return carry

    lax.fori_loop(0, nj, arrive, 0)
    for c in first:
        c.wait_send()
    for h in range(hops):
        blk = i_block(h, h + 1 == hops)
        rcopy(blk, blk, is_ring.at[h], ir_ring.at[h], down).wait_send()
        blk = i_block(h + 1, h + 1 == hops)
        rcopy(blk, blk, is_d2d.at[h], ir_d2d.at[h], partner).wait_send()

    def drain(j, carry):
        for h in range(hops):
            x_ring(j, h).wait_send()
            x_d2d(j, h + 1).wait_send()
        return carry

    lax.fori_loop(0, nj, drain, 0)


def up_kernel(dm, te_ref, x_ref, pg_ref, w1_ref, w3_ref, h_ref, xg_ref):
    @pl.when(pl.program_id(0) == 0)
    def _():
        for j in range(dm.nj):
            xg_ref[:, pl.ds(j * KC, KC)] = dot(pg_ref[...], x_ref[j].reshape(pg_ref.shape[1], KC)).astype(BF16)

    for i in range(dm.slots // TILE):
        rows = pl.ds(i * TILE, TILE)
        e = te_ref[i]
        a = dot(xg_ref[rows, :], w1_ref[e])
        g = dot(xg_ref[rows, :], w3_ref[e])
        h_ref[rows, :] = (jax.nn.silu(a) * g).astype(BF16)


def down_kernel(dm, H, WC, TE, HS, resid_ref, ew2, sw2, out_ref,
                BIG, V2A, V2B, S2A, S2B, E3, PR, RR, FR, SOUT, vsem, qs, qr, rs, rr, fs, fr):
    n = dm.n_chip
    hops = n // 2
    tok = dm.tok
    crows = 2 * tok
    nj = dm.nj
    slots = dm.slots
    n_tiles = slots // TILE
    group = n * crows
    me, chip, core, at, partner, down, up = ring_place(dm)
    V2 = (V2A, V2B)
    S2 = (S2A, S2B)

    def down_copies(j, slot):
        cols = pl.ds(pl.multiple_of(j * KC, KC), KC)
        return [pltpu.make_async_copy(ew2.at[:, :, cols], V2[slot], vsem.at[slot, 0]),
                pltpu.make_async_copy(sw2.at[:, cols], S2[slot], vsem.at[slot, 1])]

    start(down_copies(0, 0))
    start(down_copies(1, 1))
    entry_barrier((partner, down, up))

    pr_off = [448, 0, 128, 256, 384]
    assert crows == 128 and hops == 4

    def dblk(j, dest, row, size):
        return pl.ds(pl.multiple_of(j * group + dest * crows + row, tok), size)

    def q_copy(j, h):
        if h == 0:
            src, size = BIG.at[dblk(j, chip, (1 - core) * tok, tok), :], tok
        elif h == hops:
            src, size = BIG.at[dblk(j, at(-h), (1 - core) * tok, tok), :], tok
        else:
            src, size = BIG.at[dblk(j, at(-h), 0, crows), :], crows
        return rcopy(src, PR.at[j, pl.ds(pr_off[h], size), :], qs.at[h, j], qr.at[h, j], partner)

    rr_off = [0, 64, 192, 320]

    def r_copy(j, g):
        h = hops - g
        src, size = (BIG.at[dblk(j, at(h), core * tok, tok), :], tok) if g == 0 else (BIG.at[dblk(j, at(h), 0, crows), :], crows)
        return rcopy(src, RR.at[j, pl.ds(rr_off[g], size), :], rs.at[g, j], rr.at[g, j], down)

    def f_copy(j):
        return rcopy(RR.at[j, pl.ds(pl.multiple_of(rr_off[hops - 1] + (1 - core) * tok, tok), tok), :], FR.at[j], fs.at[j], fr.at[j], partner)

    def finish(j):
        q_copy(j, 0).wait_recv()
        f_copy(j).wait_recv()
        cols = pl.ds(pl.multiple_of(j * KC, KC), KC)
        routed = BIG[dblk(j, chip, core * tok, tok), :] + PR[j, pl.ds(pr_off[0], tok), :]
        routed = routed + RR[j, pl.ds(pl.multiple_of(rr_off[hops - 1] + core * tok, tok), tok), :] + FR[j]
        out_ref[:, cols] = (resid_ref[:, cols].astype(F32) + SOUT[j].astype(F32) + routed).astype(BF16)

    def turn(j):
        r_copy(j, hops - 1).wait_recv()
        f_copy(j).start()

    def relay(j, g):
        h = hops - g
        q_copy(j, h).wait_recv()
        if g == 0:
            rows = dblk(j, at(h), core * tok, tok)
            BIG[rows, :] += PR[j, pl.ds(pr_off[h], tok), :]
        else:
            r_copy(j, g - 1).wait_recv()
            rows = dblk(j, at(h), 0, crows)
            if g == 1:
                BIG[rows, :] += PR[j, pl.ds(pr_off[h], crows), :]
                hrows = dblk(j, at(h), core * tok, tok)
                BIG[hrows, :] += RR[j, pl.ds(rr_off[0], tok), :]
            else:
                BIG[rows, :] += PR[j, pl.ds(pr_off[h], crows), :] + RR[j, pl.ds(rr_off[g - 1], crows), :]
        r_copy(j, g).start()

    def ring(s, static):
        def ok(j):
            return (0 <= j < nj) if static else (j >= 0)
        for g in range(hops):
            cond(static, ok(s - 1 - g), functools.partial(relay, s - 1 - g, g))
        cond(static, ok(s - hops - 1), lambda: turn(s - hops - 1))
        cond(static, ok(s - hops - 2), lambda: finish(s - hops - 2))

    def down_step(j, slot):
        ring(j, False)
        wait(down_copies(j, slot))
        for i in range(n_tiles):
            e = dot(H[pl.ds(i * TILE, TILE), :], V2[slot][TE[i]]).astype(BF16)
            for p in range(3):
                E3[pl.ds(p * slots + i * TILE, TILE), :] = e
        for r in range(group // KC):
            rows = pl.ds(pl.multiple_of(j * group + r * KC, KC), KC)
            BIG[rows, :] = dot(WC[pl.ds(r * KC, KC), :], E3[...])
        SOUT[j] = dot(HS[...], S2[slot][...]).astype(BF16)
        for h in range(hops, -1, -1):
            q_copy(j, h).start()

        @pl.when(j + 2 < nj)
        def _():
            start(down_copies(j + 2, slot))

    def down_pair(p, carry):
        for q in range(2):
            down_step(2 * p + q, q)
        return carry

    lax.fori_loop(0, nj // 2, down_pair, 0)
    for s in range(nj, nj + hops + 2):
        ring(s, True)

    def drain(j, carry):
        for h in range(hops):
            r_copy(j, h).wait_send()
        for h in range(hops + 1):
            q_copy(j, h).wait_send()
        f_copy(j).wait_send()
        return carry

    lax.fori_loop(0, nj, drain, 0)


class Dims:
    pass


def solution(mesh):
    n_ep = mesh.shape['ep']
    tok_spec = P(('dp', 'ep'))
    expert_spec = P('ep')

    def device_fn(resid_in, expert_ids, priority, norm_gain, router_w, shared_w1, shared_w3, shared_w2, expert_w1, expert_w3, expert_w2):
        dm = Dims()
        dm.n_chip = n_ep // 2
        dm.tok, dm.hidden = resid_in.shape
        dm.top_k = expert_ids.shape[1]
        dm.local_e = expert_w1.shape[0]
        dm.ff = expert_w1.shape[2]
        dm.capacity = dm.tok * dm.top_k
        dm.nj = dm.hidden // KC
        dm.sff = shared_w1.shape[1]
        dm.slots = (dm.capacity + dm.local_e * (TILE - 1)) // TILE * TILE
        hops = dm.n_chip // 2
        assert dm.nj % 2 == 0
        nj, tok, ff, slots = dm.nj, dm.tok, dm.ff, dm.slots
        group = dm.n_chip * 2 * tok

        resid32 = resid_in.astype(F32)
        inv_rms = lax.rsqrt(jnp.mean(resid32 * resid32, axis=1, keepdims=True) + NORM_EPS)
        normed = (resid32 * inv_rms * norm_gain).astype(BF16)
        probs = jax.nn.softmax(jnp.dot(normed, router_w, preferred_element_type=F32), axis=1)
        pick = expert_ids[:, :, None] == jnp.arange(router_w.shape[1], dtype=jnp.int32)
        gates = ROUTE_SCALE * jnp.sum(jnp.where(pick, probs[:, None, :], 0.0), axis=2)
        blocks = normed.reshape(tok, nj, KC).transpose(1, 0, 2)

        def field(a, fill):
            return jnp.pad(a.astype(F32).T, ((0, KPAD - dm.top_k), (0, 0)), constant_values=fill)

        part = jnp.concatenate([field(expert_ids, -1.0), field(priority, 0.0), field(gates, 0.0)], axis=0)
        core = lax.axis_index('ep') % 2
        info = jnp.concatenate([jnp.where(core == 0, part, 0.0), jnp.where(core == 0, 0.0, part)], axis=1)

        vm = pl.BlockSpec(memory_space=pltpu.VMEM)
        sm = pl.BlockSpec(memory_space=pltpu.SMEM)
        hbm = pl.BlockSpec(memory_space=pl.ANY)
        dma = pltpu.SemaphoreType.DMA
        le = dm.local_e
        rows_all, pick_rows, mix, shared_act, tile_e = pl.pallas_call(
            functools.partial(gather_kernel, dm),
            out_shape=(jax.ShapeDtypeStruct((nj, dm.n_chip, 2 * tok, KC), BF16), jax.ShapeDtypeStruct((slots, group), BF16),
                       jax.ShapeDtypeStruct((group, 3 * slots), BF16), jax.ShapeDtypeStruct((tok, dm.sff), BF16),
                       jax.ShapeDtypeStruct((slots // TILE,), jnp.int32)),
            in_specs=[vm, vm, hbm, hbm],
            out_specs=(vm, vm, vm, vm, sm),
            scratch_shapes=[
                pltpu.VMEM((dm.n_chip, 2, 3 * KPAD, 2 * tok), F32),
                pltpu.VMEM((dm.n_chip, 2 * tok, KPAD), F32),
                pltpu.VMEM((dm.n_chip, 2 * tok, KPAD), F32),
                pltpu.VMEM((tok, 2 * dm.sff), F32),
                pltpu.VMEM((3, 2, KC, dm.sff), BF16),
                dma((2,)), dma((3, 2)),
                dma((hops, nj)), dma((hops, nj)), dma((hops, nj)), dma((hops, nj)),
                dma((hops,)), dma((hops,)), dma((hops,)), dma((hops,)), dma((2,)), dma((2,)),
            ],
            compiler_params=pltpu.CompilerParams(collective_id=0, has_side_effects=True, vmem_limit_bytes=22 << 20),
        )(blocks, info, shared_w1, shared_w3)
        h_act = pl.pallas_call(
            functools.partial(up_kernel, dm),
            out_shape=jax.ShapeDtypeStruct((slots, ff), BF16),
            grid=(ff // KC,),
            in_specs=[sm, vm, vm,
                      pl.BlockSpec((le, dm.hidden, KC), lambda c: (0, 0, c)), pl.BlockSpec((le, dm.hidden, KC), lambda c: (0, 0, c))],
            out_specs=pl.BlockSpec((slots, KC), lambda c: (0, c)),
            scratch_shapes=[pltpu.VMEM((slots, dm.hidden), BF16)],
            compiler_params=pltpu.CompilerParams(vmem_limit_bytes=30 << 20),
        )(tile_e, rows_all, pick_rows, expert_w1, expert_w3)
        return pl.pallas_call(
            functools.partial(down_kernel, dm),
            out_shape=jax.ShapeDtypeStruct((tok, dm.hidden), BF16),
            in_specs=[vm, vm, sm, vm, vm, hbm, hbm],
            out_specs=vm,
            scratch_shapes=[
                pltpu.VMEM((nj * group, KC), F32),
                pltpu.VMEM((le, ff, KC), BF16),
                pltpu.VMEM((le, ff, KC), BF16),
                pltpu.VMEM((dm.sff, KC), BF16),
                pltpu.VMEM((dm.sff, KC), BF16),
                pltpu.VMEM((3 * slots, KC), BF16),
                pltpu.VMEM((nj, 8 * tok, KC), F32),
                pltpu.VMEM((nj, 7 * tok, KC), F32),
                pltpu.VMEM((nj, tok, KC), F32),
                pltpu.VMEM((nj, tok, KC), BF16),
                dma((2, 2)),
                dma((hops + 1, nj)), dma((hops + 1, nj)), dma((hops, nj)), dma((hops, nj)), dma((nj,)), dma((nj,)),
            ],
            compiler_params=pltpu.CompilerParams(collective_id=1, has_side_effects=True, vmem_limit_bytes=38 << 20),
        )(h_act, mix, tile_e, shared_act, resid_in, expert_w2, shared_w2)

    return jax.shard_map(device_fn, mesh=mesh, in_specs=(tok_spec, tok_spec, tok_spec, P(), P(), P(), P(), P(), expert_spec, expert_spec, expert_spec), out_specs=tok_spec, check_vma=False)
```

```python
import functools

import jax
import jax.numpy as jnp
from jax import lax
from jax.experimental import pallas as pl
from jax.experimental.pallas import tpu as pltpu
from jax.sharding import PartitionSpec as P

NORM_EPS = 1e-6
ROUTE_SCALE = 16.0
KC = 256
TILE = 128
KPAD = 8
F32 = jnp.float32
BF16 = jnp.bfloat16


def dot(a, b):
    return jnp.dot(a, b, preferred_element_type=F32)


def ring_place(dm):
    n = dm.n_chip
    me = lax.axis_index("ep")
    chip = me // 2
    core = me - 2 * chip
    d = 1 - 2 * core

    def at(h):
        return lax.rem(chip + h * d + 2 * n, n)

    return me, chip, core, at, 2 * chip + 1 - core, 2 * at(1) + core, 2 * at(-1) + core


def rcopy(src, dst, ssem, rsem, dev):
    return pltpu.make_async_remote_copy(src_ref=src, dst_ref=dst, send_sem=ssem, recv_sem=rsem,
                                        device_id={"ep": dev}, device_id_type=pl.DeviceIdType.MESH)


def entry_barrier(devs):
    barrier = pltpu.get_barrier_semaphore()
    for dev in devs:
        pl.semaphore_signal(barrier, inc=1, device_id={"ep": dev}, device_id_type=pl.DeviceIdType.MESH)
    pl.semaphore_wait(barrier, len(devs))


def cond(static, pred, fn):
    if static:
        if pred:
            fn()
    else:
        pl.when(pred)(fn)


def start(copies):
    for c in copies:
        c.start()


def wait(copies):
    for c in copies:
        c.wait()


def gather_kernel(dm, b_ref, info_ref, sw1, sw3, XG, WC, HS, TE,
                  X, PG, I, SLT, GLT, SACC, WS, lsem, wsem, xs_ring, xr_ring, xs_d2d, xr_d2d, is_ring, ir_ring, is_d2d, ir_d2d, p_s, p_r):
    n = dm.n_chip
    hops = n // 2
    tok = dm.tok
    crows = 2 * tok
    nj = dm.nj
    slots = dm.slots
    n_tiles = slots // TILE
    group = n * crows
    me, chip, core, at, partner, down, up = ring_place(dm)
    half = pl.ds(pl.multiple_of(core * tok, tok), tok)
    sff = dm.sff

    def shared_copies(t):
        rows = pl.ds(t * KC, KC)
        return [pltpu.make_async_copy(src.at[rows, :], WS.at[t % 2, m], wsem.at[t % 2, m]) for m, src in enumerate((sw1, sw3))]

    def shared_stage(t):
        wait(shared_copies(t))
        x = b_ref[t]
        for m in range(2):
            for c in range(sff // KC):
                dst = pl.ds(m * sff + c * KC, KC)
                val = dot(x, WS[t % 2, m, :, pl.ds(c * KC, KC)])
                if t == 0:
                    SACC[:, dst] = val
                else:
                    SACC[:, dst] += val
        if t + 2 < nj:
            start(shared_copies(t + 2))

    for t in range(2):
        start(shared_copies(t))
    entry_barrier((partner, down, up))

    own_x = X.at[:, chip, half, :]
    own_i = I.at[chip, core]
    first = [rcopy(b_ref, own_x, p_s.at[0], p_r.at[0], partner), rcopy(info_ref, own_i, p_s.at[1], p_r.at[1], partner)]
    start(first)
    local = [pltpu.make_async_copy(b_ref, own_x, lsem.at[0]), pltpu.make_async_copy(info_ref, own_i, lsem.at[1])]
    start(local)
    wait(local)
    for c in first:
        c.wait_recv()

    def x_block(j, h, rows_half):
        return X.at[j, at(-h), half, :] if rows_half else X.at[j, at(-h)]

    def x_ring(j, h):
        blk = x_block(j, h, h + 1 == hops)
        return rcopy(blk, blk, xs_ring.at[h, j], xr_ring.at[h, j], down)

    def x_ring_in(j, h):
        blk = x_block(j, h, h == hops)
        return rcopy(blk, blk, xs_ring.at[h - 1, j], xr_ring.at[h - 1, j], down)

    def x_d2d(j, h):
        blk = x_block(j, h, h == hops)
        return rcopy(blk, blk, xs_d2d.at[h - 1, j], xr_d2d.at[h - 1, j], partner)

    def x_d2d_in(j, h):
        blk = X.at[j, at(h), pl.ds(pl.multiple_of((1 - core) * tok, tok), tok), :] if h == hops else X.at[j, at(h)]
        return rcopy(blk, blk, xs_d2d.at[h - 1, j], xr_d2d.at[h - 1, j], partner)

    def forward(h, j):
        if h > 0:
            x_ring_in(j, h).wait_recv()
        if h < hops:
            x_ring(j, h).start()
        if h > 0:
            x_d2d(j, h).start()

    def i_block(h, rows_half, sign=-1, c=None):
        return I.at[at(sign * h), core if c is None else c] if rows_half else I.at[at(sign * h)]

    def comm_info(h):
        if h > 0:
            blk = i_block(h, h == hops)
            rcopy(blk, blk, is_ring.at[h - 1], ir_ring.at[h - 1], down).wait_recv()
        if h < hops:
            blk = i_block(h, h + 1 == hops)
            rcopy(blk, blk, is_ring.at[h], ir_ring.at[h], down).start()
        if h > 0:
            blk = i_block(h, h == hops)
            rcopy(blk, blk, is_d2d.at[h - 1], ir_d2d.at[h - 1], partner).start()

    comm_info(0)
    for j in range(nj // 2):
        forward(0, j)
    comm_info(1)
    for j in range(nj // 2, nj):
        forward(0, j)
    for j in range(3):
        forward(1, j)
    shared_stage(0)
    comm_info(2)
    for j in range(3, 7):
        forward(1, j)
    shared_stage(1)
    for j in range(7, nj):
        forward(1, j)
    comm_info(3)
    shared_stage(2)
    for j in range(4):
        forward(2, j)
    comm_info(hops)

    for h in range(1, hops + 1):
        blk = i_block(h, h == hops, 1, 1 - core)
        rcopy(blk, blk, is_d2d.at[h - 1], ir_d2d.at[h - 1], partner).wait_recv()

    lanes = crows
    nr = n * KPAD

    def field(i):
        rows = pl.ds(i * KPAD, KPAD)
        return (I[:, 0, rows, :] + I[:, 1, rows, :]).reshape(nr, lanes)

    mine_e = field(0) - (me * dm.local_e).astype(F32)
    prio = field(1)
    gate = field(2)
    mine = (mine_e >= 0) & (mine_e < dm.local_e)
    key = jnp.where(mine, prio, 1e9)
    cut = jnp.zeros((1, 1), F32)
    bit = 1 << (group * dm.top_k).bit_length()
    while bit >= 1:
        cand = cut + float(bit)
        cnt = jnp.sum(jnp.where(key < cand, 1.0, 0.0), keepdims=True)
        cut = jnp.where(cnt <= float(dm.capacity), cand, cut)
        bit //= 2
    kept = key < cut
    masks = [jnp.where(kept & (mine_e == float(e)), 1.0, 0.0) for e in range(dm.local_e)]
    stack = jnp.concatenate(masks, axis=0)
    li = lax.broadcasted_iota(jnp.int32, (lanes, lanes), 0)
    lj = lax.broadcasted_iota(jnp.int32, (lanes, lanes), 1)
    upper = jnp.where(li <= lj, 1.0, 0.0).astype(BF16)
    inrow = dot(stack.astype(BF16), upper)
    total_rows = dm.local_e * nr
    rowtot = jnp.broadcast_to(inrow[:, lanes - 1:lanes], (total_rows, lanes))
    ri = lax.broadcasted_iota(jnp.int32, (total_rows, total_rows), 0)
    rj = lax.broadcasted_iota(jnp.int32, (total_rows, total_rows), 1)
    lower = jnp.where((ri > rj) & (ri // nr == rj // nr), 1.0, 0.0).astype(BF16)
    before = dot(lower, rowtot.astype(BF16))
    slot_of = jnp.full((nr, lanes), -1.0, F32)
    base = jnp.zeros((1, lanes), F32)
    bound = jnp.int32(0)
    bounds = []
    for e in range(dm.local_e):
        rows = slice(e * nr, (e + 1) * nr)
        pos = base + before[rows] + inrow[rows] - 1.0
        slot_of = jnp.where(masks[e] > 0.5, pos, slot_of)
        last = (e + 1) * nr - 1
        count = before[last:last + 1] + rowtot[last:last + 1]
        base = base + jnp.floor((count + (TILE - 1.0)) * (1.0 / TILE)) * TILE
        count_i = jnp.sum(jnp.where(kept & (mine_e == float(e)), 1, 0))
        bound = bound + (count_i + (TILE - 1)) // TILE
        bounds.append(bound)
    tile_e = [sum(jnp.where(bounds[e] <= i, 1, 0) for e in range(dm.local_e - 1)) for i in range(n_tiles)]

    slot_t = slot_of.T
    gate_t = gate.T
    for c in range(n):
        SLT[c] = slot_t[:, c * KPAD:(c + 1) * KPAD]
        GLT[c] = gate_t[:, c * KPAD:(c + 1) * KPAD]
        for r in range(n_tiles):
            srow = (lax.broadcasted_iota(jnp.int32, (TILE, lanes), 0) + r * TILE).astype(F32)
            hit = jnp.zeros((TILE, lanes), F32)
            for k in range(dm.top_k):
                hit = jnp.where(slot_of[c * KPAD + k:c * KPAD + k + 1] == srow, 1.0, hit)
            PG[pl.ds(r * TILE, TILE), pl.ds(c * lanes, lanes)] = hit.astype(BF16)

    for i in range(n_tiles):
        TE[i] = tile_e[i]
    TE[n_tiles] = bounds[dm.local_e - 1]

    def combine_rows(c):
        sl = SLT[c]
        gl = GLT[c]
        rows = pl.ds(c * crows, crows)
        for p in range(slots // KC):
            scol = (lax.broadcasted_iota(jnp.int32, (crows, KC), 1) + p * KC).astype(F32)
            w = jnp.zeros((crows, KC), F32)
            for k in range(dm.top_k):
                w = jnp.where(sl[:, k:k + 1] == scol, gl[:, k:k + 1], w)
            for i in range(3):
                part = w.astype(BF16)
                WC[rows, pl.ds(i * slots + p * KC, KC)] = part
                w = w - part.astype(F32)

    todo = [(2, j) for j in range(4, nj)] + [(3, j) for j in range(nj)]
    work = []
    for t in range(max(nj - 3, n)):
        if t < n:
            work.append(functools.partial(combine_rows, t))
        if t < nj - 3:
            work.append(functools.partial(shared_stage, t + 3))
    total = len(work)
    for u, (h, j) in enumerate(todo):
        forward(h, j)
        while len(work) > total * (len(todo) - 1 - u) // len(todo):
            work.pop(0)()
    for c in range(sff // KC):
        a = SACC[:, pl.ds(c * KC, KC)]
        g = SACC[:, pl.ds(sff + c * KC, KC)]
        HS[:, pl.ds(c * KC, KC)] = (jax.nn.silu(a) * g).astype(BF16)

    def pick(j):
        for h in range(1, hops + 1):
            x_d2d_in(j, h).wait_recv()
        XG[:, pl.ds(pl.multiple_of(j * KC, KC), KC)] = dot(PG[...], X[j].reshape(group, KC)).astype(BF16)

    lag = 3
    for j in range(lag):
        forward(hops, j)

    def last_hop(j, carry):
        forward(hops, j)
        pick(j - lag)
        return carry

    lax.fori_loop(lag, nj, last_hop, 0)

    def last_pick(j, carry):
        pick(j)
        return carry

    lax.fori_loop(nj - lag, nj, last_pick, 0)

    for c in first:
        c.wait_send()
    for h in range(hops):
        blk = i_block(h, h + 1 == hops)
        rcopy(blk, blk, is_ring.at[h], ir_ring.at[h], down).wait_send()
        blk = i_block(h + 1, h + 1 == hops)
        rcopy(blk, blk, is_d2d.at[h], ir_d2d.at[h], partner).wait_send()

    def drain(j, carry):
        for h in range(hops):
            x_ring(j, h).wait_send()
            x_d2d(j, h + 1).wait_send()
        return carry

    lax.fori_loop(0, nj, drain, 0)


def up_kernel(dm, te_ref, xg_ref, w1_ref, w3_ref, h_ref):
    n_tiles = dm.slots // TILE
    for i in range(n_tiles):
        rows = pl.ds(i * TILE, TILE)

        @pl.when(i < te_ref[n_tiles])
        def _():
            e = te_ref[i]
            a = dot(xg_ref[rows, :], w1_ref[e])
            g = dot(xg_ref[rows, :], w3_ref[e])
            h_ref[rows, :] = (jax.nn.silu(a) * g).astype(BF16)

        @pl.when(i >= te_ref[n_tiles])
        def _():
            h_ref[rows, :] = jnp.zeros((TILE, KC), BF16)


def down_kernel(dm, H, WC, TE, HS, resid_ref, ew2, sw2, out_ref,
                BIG, V2A, V2B, S2A, S2B, E3, PR, RR, FR, SOUT, vsem, qs, qr, rs, rr, fs, fr):
    n = dm.n_chip
    hops = n // 2
    tok = dm.tok
    crows = 2 * tok
    nj = dm.nj
    slots = dm.slots
    n_tiles = slots // TILE
    group = n * crows
    me, chip, core, at, partner, down, up = ring_place(dm)
    V2 = (V2A, V2B)
    S2 = (S2A, S2B)

    def down_copies(j, slot):
        cols = pl.ds(pl.multiple_of(j * KC, KC), KC)
        return [pltpu.make_async_copy(ew2.at[:, :, cols], V2[slot], vsem.at[slot, 0]),
                pltpu.make_async_copy(sw2.at[:, cols], S2[slot], vsem.at[slot, 1])]

    start(down_copies(0, 0))
    start(down_copies(1, 1))
    entry_barrier((partner, down, up))

    pr_off = [448, 0, 128, 256, 384]
    assert crows == 128 and hops == 4

    def dblk(j, dest, row, size):
        return pl.ds(pl.multiple_of(j * group + dest * crows + row, tok), size)

    def q_copy(j, h):
        if h == 0:
            src, size = BIG.at[dblk(j, chip, (1 - core) * tok, tok), :], tok
        elif h == hops:
            src, size = BIG.at[dblk(j, at(-h), (1 - core) * tok, tok), :], tok
        else:
            src, size = BIG.at[dblk(j, at(-h), 0, crows), :], crows
        return rcopy(src, PR.at[j, pl.ds(pr_off[h], size), :], qs.at[h, j], qr.at[h, j], partner)

    rr_off = [0, 64, 192, 320]

    def r_copy(j, g):
        h = hops - g
        src, size = (BIG.at[dblk(j, at(h), core * tok, tok), :], tok) if g == 0 else (BIG.at[dblk(j, at(h), 0, crows), :], crows)
        return rcopy(src, RR.at[j, pl.ds(rr_off[g], size), :], rs.at[g, j], rr.at[g, j], down)

    def f_copy(j):
        return rcopy(RR.at[j, pl.ds(pl.multiple_of(rr_off[hops - 1] + (1 - core) * tok, tok), tok), :], FR.at[j], fs.at[j], fr.at[j], partner)

    def finish(j):
        q_copy(j, 0).wait_recv()
        f_copy(j).wait_recv()
        cols = pl.ds(pl.multiple_of(j * KC, KC), KC)
        routed = BIG[dblk(j, chip, core * tok, tok), :] + PR[j, pl.ds(pr_off[0], tok), :]
        routed = routed + RR[j, pl.ds(pl.multiple_of(rr_off[hops - 1] + core * tok, tok), tok), :] + FR[j]
        out_ref[:, cols] = (resid_ref[:, cols].astype(F32) + SOUT[j].astype(F32) + routed).astype(BF16)

    def turn(j):
        r_copy(j, hops - 1).wait_recv()
        f_copy(j).start()

    def relay(j, g):
        h = hops - g
        q_copy(j, h).wait_recv()
        if g == 0:
            rows = dblk(j, at(h), core * tok, tok)
            BIG[rows, :] += PR[j, pl.ds(pr_off[h], tok), :]
        else:
            r_copy(j, g - 1).wait_recv()
            rows = dblk(j, at(h), 0, crows)
            if g == 1:
                BIG[rows, :] += PR[j, pl.ds(pr_off[h], crows), :]
                hrows = dblk(j, at(h), core * tok, tok)
                BIG[hrows, :] += RR[j, pl.ds(rr_off[0], tok), :]
            else:
                BIG[rows, :] += PR[j, pl.ds(pr_off[h], crows), :] + RR[j, pl.ds(rr_off[g - 1], crows), :]
        r_copy(j, g).start()

    skew = 2

    def ring(s, static):
        def ok(j):
            return (0 <= j < nj) if static else (j >= 0)
        for g in range(1, hops):
            cond(static, ok(s - 1 - skew * g), functools.partial(relay, s - 1 - skew * g, g))
        cond(static, ok(s - 1), functools.partial(relay, s - 1, 0))
        cond(static, ok(s - 1 - skew * hops), lambda: turn(s - 1 - skew * hops))
        cond(static, ok(s - 2 - skew * hops), lambda: finish(s - 2 - skew * hops))

    def down_step(j, slot):
        ring(j, False)
        wait(down_copies(j, slot))
        for i in range(n_tiles):
            e = dot(H[pl.ds(i * TILE, TILE), :], V2[slot][TE[i]]).astype(BF16)
            for p in range(3):
                E3[pl.ds(p * slots + i * TILE, TILE), :] = e
        for r in range(group // KC):
            rows = pl.ds(pl.multiple_of(j * group + r * KC, KC), KC)
            BIG[rows, :] = dot(WC[pl.ds(r * KC, KC), :], E3[...])
        for h in range(hops, -1, -1):
            q_copy(j, h).start()
        SOUT[j] = dot(HS[...], S2[slot][...]).astype(BF16)

        @pl.when(j + 2 < nj)
        def _():
            start(down_copies(j + 2, slot))

    def down_pair(p, carry):
        for q in range(2):
            down_step(2 * p + q, q)
        return carry

    lax.fori_loop(0, nj // 2, down_pair, 0)
    for s in range(nj, nj + skew * hops + 2):
        ring(s, True)

    def drain(j, carry):
        for h in range(hops):
            r_copy(j, h).wait_send()
        for h in range(hops + 1):
            q_copy(j, h).wait_send()
        f_copy(j).wait_send()
        return carry

    lax.fori_loop(0, nj, drain, 0)


class Dims:
    pass


def solution(mesh):
    n_ep = mesh.shape['ep']
    tok_spec = P(('dp', 'ep'))
    expert_spec = P('ep')

    def device_fn(resid_in, expert_ids, priority, norm_gain, router_w, shared_w1, shared_w3, shared_w2, expert_w1, expert_w3, expert_w2):
        dm = Dims()
        dm.n_chip = n_ep // 2
        dm.tok, dm.hidden = resid_in.shape
        dm.top_k = expert_ids.shape[1]
        dm.local_e = expert_w1.shape[0]
        dm.ff = expert_w1.shape[2]
        dm.capacity = dm.tok * dm.top_k
        dm.nj = dm.hidden // KC
        dm.sff = shared_w1.shape[1]
        dm.slots = (dm.capacity + dm.local_e * (TILE - 1)) // TILE * TILE
        hops = dm.n_chip // 2
        assert dm.nj % 2 == 0
        nj, tok, ff, slots = dm.nj, dm.tok, dm.ff, dm.slots
        group = dm.n_chip * 2 * tok

        resid32 = resid_in.astype(F32)
        inv_rms = lax.rsqrt(jnp.mean(resid32 * resid32, axis=1, keepdims=True) + NORM_EPS)
        normed = (resid32 * inv_rms * norm_gain).astype(BF16)
        probs = jax.nn.softmax(jnp.dot(normed, router_w, preferred_element_type=F32), axis=1)
        pick = expert_ids[:, :, None] == jnp.arange(router_w.shape[1], dtype=jnp.int32)
        gates = ROUTE_SCALE * jnp.sum(jnp.where(pick, probs[:, None, :], 0.0), axis=2)
        blocks = normed.reshape(tok, nj, KC).transpose(1, 0, 2)

        def field(a, fill):
            return jnp.pad(a.astype(F32).T, ((0, KPAD - dm.top_k), (0, 0)), constant_values=fill)

        part = jnp.concatenate([field(expert_ids, -1.0), field(priority, 0.0), field(gates, 0.0)], axis=0)
        core = lax.axis_index('ep') % 2
        info = jnp.concatenate([jnp.where(core == 0, part, 0.0), jnp.where(core == 0, 0.0, part)], axis=1)

        vm = pl.BlockSpec(memory_space=pltpu.VMEM)
        sm = pl.BlockSpec(memory_space=pltpu.SMEM)
        hbm = pl.BlockSpec(memory_space=pltpu.HBM)
        dma = pltpu.SemaphoreType.DMA
        le = dm.local_e
        picked, mix, shared_act, tile_e = pl.pallas_call(
            functools.partial(gather_kernel, dm),
            out_shape=(jax.ShapeDtypeStruct((slots, dm.hidden), BF16),
                       jax.ShapeDtypeStruct((group, 3 * slots), BF16), jax.ShapeDtypeStruct((tok, dm.sff), BF16),
                       jax.ShapeDtypeStruct((slots // TILE + 1,), jnp.int32)),
            in_specs=[vm, vm, hbm, hbm],
            out_specs=(vm, vm, vm, sm),
            scratch_shapes=[
                pltpu.VMEM((nj, dm.n_chip, 2 * tok, KC), BF16),
                pltpu.VMEM((slots, group), BF16),
                pltpu.VMEM((dm.n_chip, 2, 3 * KPAD, 2 * tok), F32),
                pltpu.VMEM((dm.n_chip, 2 * tok, KPAD), F32),
                pltpu.VMEM((dm.n_chip, 2 * tok, KPAD), F32),
                pltpu.VMEM((tok, 2 * dm.sff), F32),
                pltpu.VMEM((2, 2, KC, dm.sff), BF16),
                dma((2,)), dma((2, 2)),
                dma((hops, nj)), dma((hops, nj)), dma((hops, nj)), dma((hops, nj)),
                dma((hops,)), dma((hops,)), dma((hops,)), dma((hops,)), dma((2,)), dma((2,)),
            ],
            compiler_params=pltpu.CompilerParams(collective_id=0, has_side_effects=True, vmem_limit_bytes=46 << 20),
            cost_estimate=pl.CostEstimate(flops=35_000_000_000, bytes_accessed=40_000_000, transcendentals=0),
        )(blocks, info, shared_w1, shared_w3)
        h_act = pl.pallas_call(
            functools.partial(up_kernel, dm),
            out_shape=jax.ShapeDtypeStruct((slots, ff), BF16),
            grid=(ff // KC,),
            in_specs=[sm, vm,
                      pl.BlockSpec((le, dm.hidden, KC), lambda c: (0, 0, c)), pl.BlockSpec((le, dm.hidden, KC), lambda c: (0, 0, c))],
            out_specs=pl.BlockSpec((slots, KC), lambda c: (0, c)),
            compiler_params=pltpu.CompilerParams(vmem_limit_bytes=44 << 20),
            cost_estimate=pl.CostEstimate(flops=10_000_000_000, bytes_accessed=70_000_000, transcendentals=0),
        )(tile_e, picked, expert_w1, expert_w3)
        return pl.pallas_call(
            functools.partial(down_kernel, dm),
            out_shape=jax.ShapeDtypeStruct((tok, dm.hidden), BF16),
            in_specs=[vm, vm, sm, vm, vm, hbm, hbm],
            out_specs=vm,
            scratch_shapes=[
                pltpu.VMEM((nj * group, KC), F32),
                pltpu.VMEM((le, ff, KC), BF16),
                pltpu.VMEM((le, ff, KC), BF16),
                pltpu.VMEM((dm.sff, KC), BF16),
                pltpu.VMEM((dm.sff, KC), BF16),
                pltpu.VMEM((3 * slots, KC), BF16),
                pltpu.VMEM((nj, 8 * tok, KC), F32),
                pltpu.VMEM((nj, 7 * tok, KC), F32),
                pltpu.VMEM((nj, tok, KC), F32),
                pltpu.VMEM((nj, tok, KC), BF16),
                dma((2, 2)),
                dma((hops + 1, nj)), dma((hops + 1, nj)), dma((hops, nj)), dma((hops, nj)), dma((nj,)), dma((nj,)),
            ],
            compiler_params=pltpu.CompilerParams(collective_id=1, has_side_effects=True, vmem_limit_bytes=38 << 20),
        )(h_act, mix, tile_e, shared_act, resid_in, expert_w2, shared_w2)

    return jax.shard_map(device_fn, mesh=mesh, in_specs=(tok_spec, tok_spec, tok_spec, P(), P(), P(), P(), P(), expert_spec, expert_spec, expert_spec), out_specs=tok_spec, check_vma=False)
```

```python
import functools

import jax
import jax.numpy as jnp
from jax import lax
from jax.experimental import pallas as pl
from jax.experimental.pallas import tpu as pltpu
from jax.sharding import PartitionSpec as P

NORM_EPS = 1e-6
ROUTE_SCALE = 16.0
KC = 256
TILE = 128
KPAD = 8
F32 = jnp.float32
BF16 = jnp.bfloat16


def dot(a, b):
    return jnp.dot(a, b, preferred_element_type=F32)


def ring_place(dm):
    n = dm.n_chip
    me = lax.axis_index("ep")
    chip = me // 2
    core = me - 2 * chip
    d = 1 - 2 * core

    def at(h):
        return lax.rem(chip + h * d + 2 * n, n)

    return me, chip, core, at, 2 * chip + 1 - core, 2 * at(1) + core, 2 * at(-1) + core


def rcopy(src, dst, ssem, rsem, dev):
    return pltpu.make_async_remote_copy(src_ref=src, dst_ref=dst, send_sem=ssem, recv_sem=rsem,
                                        device_id={"ep": dev}, device_id_type=pl.DeviceIdType.MESH)


def entry_signal(devs):
    barrier = pltpu.get_barrier_semaphore()
    for dev in devs:
        pl.semaphore_signal(barrier, inc=1, device_id={"ep": dev}, device_id_type=pl.DeviceIdType.MESH)


def entry_wait(count):
    pl.semaphore_wait(pltpu.get_barrier_semaphore(), count)


def entry_barrier(devs):
    entry_signal(devs)
    entry_wait(len(devs))


def cond(static, pred, fn):
    if static:
        if pred:
            fn()
    else:
        pl.when(pred)(fn)


def start(copies):
    for c in copies:
        c.start()


def wait(copies):
    for c in copies:
        c.wait()


def gather_kernel(dm, resid_ref, gain_ref, router_ref, ids_ref, prio_ref, sw1, sw3, X, PG, WC, HS, TE,
                  B, I, SLT, GLT, SACC, WS, wsem, xs_other, xr_other, xs_ring, xr_ring, xs_d2d, xr_d2d, is_ring, ir_ring, is_d2d, ir_d2d, p_s, p_r):
    n = dm.n_chip
    hops = n // 2
    tok = dm.tok
    crows = 2 * tok
    nj = dm.nj
    slots = dm.slots
    n_tiles = slots // TILE
    group = n * crows
    me, chip, core, at, partner, down, up = ring_place(dm)
    half = pl.ds(pl.multiple_of(core * tok, tok), tok)
    sff = dm.sff

    def shared_copies(t):
        rows = pl.ds(t * KC, KC)
        return [pltpu.make_async_copy(src.at[rows, :], WS.at[t % 2, m], wsem.at[t % 2, m]) for m, src in enumerate((sw1, sw3))]

    def shared_stage(t):
        wait(shared_copies(t))
        x = B[t]
        for m in range(2):
            for c in range(sff // KC):
                dst = pl.ds(m * sff + c * KC, KC)
                val = dot(x, WS[t % 2, m, :, pl.ds(c * KC, KC)])
                if t == 0:
                    SACC[:, dst] = val
                else:
                    SACC[:, dst] += val
        if t + 2 < nj:
            start(shared_copies(t + 2))

    for t in range(2):
        start(shared_copies(t))
    entry_signal((partner, down, up))

    resid32 = resid_ref[...].astype(F32)
    inv_rms = lax.rsqrt(jnp.mean(resid32 * resid32, axis=1, keepdims=True) + NORM_EPS)
    normed = (resid32 * inv_rms * gain_ref[...]).astype(BF16)
    for j in range(nj):
        B[j] = normed[:, j * KC:(j + 1) * KC]
        X[j, chip, half, :] = normed[:, j * KC:(j + 1) * KC]
    logits = lax.dot_general(router_ref[...], normed, (((1,), (1,)), ((), ())), preferred_element_type=F32)
    powers = jnp.exp(logits - jnp.max(logits, axis=0, keepdims=True))
    probs = powers / jnp.sum(powers, axis=0, keepdims=True)
    experts = lax.broadcasted_iota(jnp.int32, probs.shape, 0)
    ids = ids_ref[...]

    def put(i, k, row):
        zero = jnp.zeros((1, tok), F32)
        I[chip, core, pl.ds(i * KPAD + k, 1), :] = jnp.where(core == 0, jnp.concatenate([row, zero], axis=1), jnp.concatenate([zero, row], axis=1))

    for k in range(KPAD):
        if k < dm.top_k:
            put(0, k, ids[k:k + 1].astype(F32))
            put(1, k, prio_ref[k:k + 1, :].astype(F32))
            put(2, k, ROUTE_SCALE * jnp.sum(jnp.where(experts == ids[k:k + 1], probs, 0.0), axis=0, keepdims=True))
        else:
            put(0, k, jnp.full((1, tok), -1.0, F32))
            put(1, k, jnp.zeros((1, tok), F32))
            put(2, k, jnp.zeros((1, tok), F32))

    entry_wait(3)
    own_x = X.at[:, chip, half, :]
    own_i = I.at[chip, core]
    first = [rcopy(own_i, own_i, p_s.at[1], p_r.at[1], partner), rcopy(own_x, own_x, p_s.at[0], p_r.at[0], partner)]
    start(first)

    def x_block(j, h, rows_half):
        return X.at[j, at(-h), half, :] if rows_half else X.at[j, at(-h)]

    def x_ring(j, h):
        blk = x_block(j, h, h + 1 == hops)
        return rcopy(blk, blk, xs_ring.at[h, j], xr_ring.at[h, j], down)

    def x_ring_in(j, h):
        blk = x_block(j, h, h == hops)
        return rcopy(blk, blk, xs_ring.at[h - 1, j], xr_ring.at[h - 1, j], down)

    def x_d2d(j, h):
        blk = x_block(j, h, h == hops)
        return rcopy(blk, blk, xs_d2d.at[h - 1, j], xr_d2d.at[h - 1, j], partner)

    def x_d2d_in(j, h):
        blk = X.at[j, at(h), pl.ds(pl.multiple_of((1 - core) * tok, tok), tok), :] if h == hops else X.at[j, at(h)]
        return rcopy(blk, blk, xs_d2d.at[h - 1, j], xr_d2d.at[h - 1, j], partner)

    def x_part(j, h, other):
        rows = pl.ds(pl.multiple_of((1 - core) * tok, tok), tok) if other else half
        blk = X.at[j, at(-h), rows, :]
        return rcopy(blk, blk, xs_other.at[j], xr_other.at[j], down) if other else rcopy(blk, blk, xs_ring.at[0, j], xr_ring.at[0, j], down)

    def forward(h, j):
        if h == 1:
            x_part(j, 1, False).wait_recv()
            x_part(j, 1, True).wait_recv()
        elif h > 1:
            x_ring_in(j, h).wait_recv()
        if h < hops:
            x_ring(j, h).start()
        if h > 0:
            x_d2d(j, h).start()

    def i_block(h, rows_half, sign=-1, c=None):
        return I.at[at(sign * h), core if c is None else c] if rows_half else I.at[at(sign * h)]

    def comm_info(h):
        if h > 0:
            blk = i_block(h, h == hops)
            rcopy(blk, blk, is_ring.at[h - 1], ir_ring.at[h - 1], down).wait_recv()
        if h < hops:
            blk = i_block(h, h + 1 == hops)
            rcopy(blk, blk, is_ring.at[h], ir_ring.at[h], down).start()
        if h > 0:
            blk = i_block(h, h == hops)
            rcopy(blk, blk, is_d2d.at[h - 1], ir_d2d.at[h - 1], partner).start()

    for j in range(nj // 2):
        x_part(j, 0, False).start()
    first[0].wait_recv()
    comm_info(0)
    for j in range(nj // 2, nj):
        x_part(j, 0, False).start()
    first[1].wait_recv()
    for j in range(nj // 2):
        x_part(j, 0, True).start()
    comm_info(1)
    for j in range(nj // 2, nj):
        x_part(j, 0, True).start()
    for j in range(3):
        forward(1, j)
    shared_stage(0)
    comm_info(2)
    for j in range(3, 7):
        forward(1, j)
    shared_stage(1)
    for j in range(7, nj):
        forward(1, j)
    comm_info(3)
    shared_stage(2)
    for j in range(4):
        forward(2, j)
    comm_info(hops)

    for h in range(1, hops + 1):
        blk = i_block(h, h == hops, 1, 1 - core)
        rcopy(blk, blk, is_d2d.at[h - 1], ir_d2d.at[h - 1], partner).wait_recv()

    lanes = crows
    nr = n * KPAD

    def field(i):
        rows = pl.ds(i * KPAD, KPAD)
        return (I[:, 0, rows, :] + I[:, 1, rows, :]).reshape(nr, lanes)

    mine_e = field(0) - (me * dm.local_e).astype(F32)
    prio = field(1)
    gate = field(2)
    mine = (mine_e >= 0) & (mine_e < dm.local_e)
    key = jnp.where(mine, prio, 1e9)
    cut = jnp.zeros((1, 1), F32)
    bit = 1 << (group * dm.top_k).bit_length()
    while bit >= 1:
        cand = cut + float(bit)
        cnt = jnp.sum(jnp.where(key < cand, 1.0, 0.0), keepdims=True)
        cut = jnp.where(cnt <= float(dm.capacity), cand, cut)
        bit //= 2
    kept = key < cut
    masks = [jnp.where(kept & (mine_e == float(e)), 1.0, 0.0) for e in range(dm.local_e)]
    stack = jnp.concatenate(masks, axis=0)
    li = lax.broadcasted_iota(jnp.int32, (lanes, lanes), 0)
    lj = lax.broadcasted_iota(jnp.int32, (lanes, lanes), 1)
    upper = jnp.where(li <= lj, 1.0, 0.0).astype(BF16)
    inrow = dot(stack.astype(BF16), upper)
    total_rows = dm.local_e * nr
    rowtot = jnp.broadcast_to(inrow[:, lanes - 1:lanes], (total_rows, lanes))
    ri = lax.broadcasted_iota(jnp.int32, (total_rows, total_rows), 0)
    rj = lax.broadcasted_iota(jnp.int32, (total_rows, total_rows), 1)
    lower = jnp.where((ri > rj) & (ri // nr == rj // nr), 1.0, 0.0).astype(BF16)
    before = dot(lower, rowtot.astype(BF16))
    slot_of = jnp.full((nr, lanes), -1.0, F32)
    base = jnp.zeros((1, lanes), F32)
    bound = jnp.int32(0)
    bounds = []
    for e in range(dm.local_e):
        rows = slice(e * nr, (e + 1) * nr)
        pos = base + before[rows] + inrow[rows] - 1.0
        slot_of = jnp.where(masks[e] > 0.5, pos, slot_of)
        last = (e + 1) * nr - 1
        count = before[last:last + 1] + rowtot[last:last + 1]
        base = base + jnp.floor((count + (TILE - 1.0)) * (1.0 / TILE)) * TILE
        count_i = jnp.sum(jnp.where(kept & (mine_e == float(e)), 1, 0))
        bound = bound + (count_i + (TILE - 1)) // TILE
        bounds.append(bound)
    tile_e = [sum(jnp.where(bounds[e] <= i, 1, 0) for e in range(dm.local_e - 1)) for i in range(n_tiles)]

    slot_t = slot_of.T
    gate_t = gate.T
    for c in range(n):
        SLT[c] = slot_t[:, c * KPAD:(c + 1) * KPAD]
        GLT[c] = gate_t[:, c * KPAD:(c + 1) * KPAD]
        for r in range(n_tiles):
            srow = (lax.broadcasted_iota(jnp.int32, (TILE, lanes), 0) + r * TILE).astype(F32)
            hit = jnp.zeros((TILE, lanes), F32)
            for k in range(dm.top_k):
                hit = jnp.where(slot_of[c * KPAD + k:c * KPAD + k + 1] == srow, 1.0, hit)
            PG[pl.ds(r * TILE, TILE), pl.ds(c * lanes, lanes)] = hit.astype(BF16)

    for i in range(n_tiles):
        TE[i] = tile_e[i]
    TE[n_tiles] = bounds[dm.local_e - 1]

    def combine_rows(c):
        sl = SLT[c]
        gl = GLT[c]
        rows = pl.ds(c * crows, crows)
        for p in range(slots // KC):
            scol = (lax.broadcasted_iota(jnp.int32, (crows, KC), 1) + p * KC).astype(F32)
            w = jnp.zeros((crows, KC), F32)
            for k in range(dm.top_k):
                w = jnp.where(sl[:, k:k + 1] == scol, gl[:, k:k + 1], w)
            for i in range(3):
                part = w.astype(BF16)
                WC[rows, pl.ds(i * slots + p * KC, KC)] = part
                w = w - part.astype(F32)

    todo = [(2, j) for j in range(4, nj)] + [(3, j) for j in range(nj)]
    work = []
    for t in range(max(nj - 3, n)):
        if t < n:
            work.append(functools.partial(combine_rows, t))
        if t < nj - 3:
            work.append(functools.partial(shared_stage, t + 3))
    total = len(work)
    for u, (h, j) in enumerate(todo):
        forward(h, j)
        while len(work) > total * (len(todo) - 1 - u) // len(todo):
            work.pop(0)()
    for c in range(sff // KC):
        a = SACC[:, pl.ds(c * KC, KC)]
        g = SACC[:, pl.ds(sff + c * KC, KC)]
        HS[:, pl.ds(c * KC, KC)] = (jax.nn.silu(a) * g).astype(BF16)

    def last_hop(j, carry):
        forward(hops, j)
        return carry

    lax.fori_loop(0, nj, last_hop, 0)

    def arrive(j, carry):
        for h in range(1, hops + 1):
            x_d2d_in(j, h).wait_recv()
        return carry

    lax.fori_loop(0, nj, arrive, 0)
    for c in first:
        c.wait_send()
    for h in range(hops):
        blk = i_block(h, h + 1 == hops)
        rcopy(blk, blk, is_ring.at[h], ir_ring.at[h], down).wait_send()
        blk = i_block(h + 1, h + 1 == hops)
        rcopy(blk, blk, is_d2d.at[h], ir_d2d.at[h], partner).wait_send()

    def drain(j, carry):
        x_part(j, 0, False).wait_send()
        x_part(j, 0, True).wait_send()
        for h in range(hops):
            if h > 0:
                x_ring(j, h).wait_send()
            x_d2d(j, h + 1).wait_send()
        return carry

    lax.fori_loop(0, nj, drain, 0)


def up_kernel(dm, te_ref, x_ref, pg_ref, w1, w3, h_ref, xg_ref, w_ref, wsem):
    n_tiles = dm.slots // TILE
    nt = dm.ff // KC

    def copies(c, slot):
        cols = pl.ds(pl.multiple_of(c * KC, KC), KC)
        return [pltpu.make_async_copy(src.at[:, :, cols], w_ref.at[slot, m], wsem.at[slot, m]) for m, src in enumerate((w1, w3))]

    start(copies(0, 0))
    start(copies(1, 1))

    def pick(j, carry):
        xg_ref[:, pl.ds(pl.multiple_of(j * KC, KC), KC)] = dot(pg_ref[...], x_ref[j].reshape(pg_ref.shape[1], KC)).astype(BF16)
        return carry

    lax.fori_loop(0, dm.nj, pick, 0)

    def column(c, carry):
        slot = c % 2
        cols = pl.ds(pl.multiple_of(c * KC, KC), KC)
        wait(copies(c, slot))
        for i in range(n_tiles):
            rows = pl.ds(i * TILE, TILE)

            @pl.when(i < te_ref[n_tiles])
            def _():
                e = te_ref[i]
                a = dot(xg_ref[rows, :], w_ref[slot, 0, e])
                g = dot(xg_ref[rows, :], w_ref[slot, 1, e])
                h_ref[rows, cols] = (jax.nn.silu(a) * g).astype(BF16)

            @pl.when(i >= te_ref[n_tiles])
            def _():
                h_ref[rows, cols] = jnp.zeros((TILE, KC), BF16)

        @pl.when(c + 2 < nt)
        def _():
            start(copies(c + 2, slot))
        return carry

    lax.fori_loop(0, nt, column, 0)


def down_kernel(dm, H, WC, TE, HS, resid_ref, ew2, sw2, out_ref,
                BIG, V2A, V2B, S2A, S2B, E3, PR, RR, FR, SOUT, vsem, qs, qr, rs, rr, fs, fr):
    n = dm.n_chip
    hops = n // 2
    tok = dm.tok
    crows = 2 * tok
    nj = dm.nj
    slots = dm.slots
    n_tiles = slots // TILE
    group = n * crows
    me, chip, core, at, partner, down, up = ring_place(dm)
    V2 = (V2A, V2B)
    S2 = (S2A, S2B)

    def down_copies(j, slot):
        cols = pl.ds(pl.multiple_of(j * KC, KC), KC)
        return [pltpu.make_async_copy(ew2.at[:, :, cols], V2[slot], vsem.at[slot, 0])]

    def shared_copies(j, slot):
        cols = pl.ds(pl.multiple_of(j * KC, KC), KC)
        return [pltpu.make_async_copy(sw2.at[:, cols], S2[slot], vsem.at[slot, 1])]

    def shared_step(j, slot, more):
        wait(shared_copies(j, slot))
        SOUT[j] = dot(HS[...], S2[slot][...]).astype(BF16)
        if more:
            start(shared_copies(j + 2, slot))

    start(down_copies(0, 0))
    start(down_copies(1, 1))
    start(shared_copies(0, 0))
    start(shared_copies(1, 1))
    entry_barrier((partner, down, up))

    pr_off = [448, 0, 128, 256, 384]
    assert crows == 128 and hops == 4

    def dblk(j, dest, row, size):
        return pl.ds(pl.multiple_of(j * group + dest * crows + row, tok), size)

    def q_copy(j, h):
        if h == 0:
            src, size = BIG.at[dblk(j, chip, (1 - core) * tok, tok), :], tok
        elif h == hops:
            src, size = BIG.at[dblk(j, at(-h), (1 - core) * tok, tok), :], tok
        else:
            src, size = BIG.at[dblk(j, at(-h), 0, crows), :], crows
        return rcopy(src, PR.at[j, pl.ds(pr_off[h], size), :], qs.at[h, j], qr.at[h, j], partner)

    rr_off = [0, 64, 192, 320]

    def r_copy(j, g):
        h = hops - g
        src, size = (BIG.at[dblk(j, at(h), core * tok, tok), :], tok) if g == 0 else (BIG.at[dblk(j, at(h), 0, crows), :], crows)
        return rcopy(src, RR.at[j, pl.ds(rr_off[g], size), :], rs.at[g, j], rr.at[g, j], down)

    def f_copy(j):
        return rcopy(RR.at[j, pl.ds(pl.multiple_of(rr_off[hops - 1] + (1 - core) * tok, tok), tok), :], FR.at[j], fs.at[j], fr.at[j], partner)

    def finish(j):
        q_copy(j, 0).wait_recv()
        f_copy(j).wait_recv()
        cols = pl.ds(pl.multiple_of(j * KC, KC), KC)
        routed = BIG[dblk(j, chip, core * tok, tok), :] + PR[j, pl.ds(pr_off[0], tok), :]
        routed = routed + RR[j, pl.ds(pl.multiple_of(rr_off[hops - 1] + core * tok, tok), tok), :] + FR[j]
        out_ref[:, cols] = (resid_ref[:, cols].astype(F32) + SOUT[j].astype(F32) + routed).astype(BF16)

    def turn(j):
        r_copy(j, hops - 1).wait_recv()
        f_copy(j).start()

    def relay(j, g):
        h = hops - g
        q_copy(j, h).wait_recv()
        if g == 0:
            rows = dblk(j, at(h), core * tok, tok)
            BIG[rows, :] += PR[j, pl.ds(pr_off[h], tok), :]
        else:
            r_copy(j, g - 1).wait_recv()
            rows = dblk(j, at(h), 0, crows)
            if g == 1:
                BIG[rows, :] += PR[j, pl.ds(pr_off[h], crows), :]
                hrows = dblk(j, at(h), core * tok, tok)
                BIG[hrows, :] += RR[j, pl.ds(rr_off[0], tok), :]
            else:
                BIG[rows, :] += PR[j, pl.ds(pr_off[h], crows), :] + RR[j, pl.ds(rr_off[g - 1], crows), :]
        r_copy(j, g).start()

    skew = 2
    late = nj // 2

    def ring(s, static):
        def ok(j):
            return (0 <= j < nj) if static else (j >= 0)
        for g in range(1, hops):
            cond(static, ok(s - 1 - skew * g), functools.partial(relay, s - 1 - skew * g, g))
        cond(static, ok(s - 1), functools.partial(relay, s - 1, 0))
        cond(static, ok(s - 1 - skew * hops), lambda: turn(s - 1 - skew * hops))
        cond(static, ok(s - 2 - skew * hops), lambda: finish(s - 2 - skew * hops))

    def down_step(j, slot):
        ring(j, False)
        wait(down_copies(j, slot))
        for i in range(n_tiles):
            e = dot(H[pl.ds(i * TILE, TILE), :], V2[slot][TE[i]]).astype(BF16)
            for p in range(3):
                E3[pl.ds(p * slots + i * TILE, TILE), :] = e
        for r in range(group // KC):
            rows = pl.ds(pl.multiple_of(j * group + r * KC, KC), KC)
            BIG[rows, :] = dot(WC[pl.ds(r * KC, KC), :], E3[...])
        for h in range(hops, -1, -1):
            q_copy(j, h).start()

        @pl.when(j + 2 < nj)
        def _():
            start(down_copies(j + 2, slot))

        @pl.when(j >= late)
        def _():
            shared_step(j - late, (slot + late) % 2, True)

    def down_pair(p, carry):
        for q in range(2):
            down_step(2 * p + q, q)
        return carry

    lax.fori_loop(0, nj // 2, down_pair, 0)
    for s in range(nj, nj + skew * hops + 2):
        ring(s, True)
        if 0 <= s - late < nj:
            shared_step(s - late, (s - late) % 2, s - late + 2 < nj)

    def drain(j, carry):
        for h in range(hops):
            r_copy(j, h).wait_send()
        for h in range(hops + 1):
            q_copy(j, h).wait_send()
        f_copy(j).wait_send()
        return carry

    lax.fori_loop(0, nj, drain, 0)


class Dims:
    pass


def solution(mesh):
    n_ep = mesh.shape['ep']
    tok_spec = P(('dp', 'ep'))
    expert_spec = P('ep')

    def device_fn(resid_in, expert_ids, priority, norm_gain, router_w, shared_w1, shared_w3, shared_w2, expert_w1, expert_w3, expert_w2):
        dm = Dims()
        dm.n_chip = n_ep // 2
        dm.tok, dm.hidden = resid_in.shape
        dm.top_k = expert_ids.shape[1]
        dm.local_e = expert_w1.shape[0]
        dm.ff = expert_w1.shape[2]
        dm.capacity = dm.tok * dm.top_k
        dm.nj = dm.hidden // KC
        dm.sff = shared_w1.shape[1]
        dm.slots = (dm.capacity + dm.local_e * (TILE - 1)) // TILE * TILE
        hops = dm.n_chip // 2
        assert dm.nj % 2 == 0
        nj, tok, ff, slots = dm.nj, dm.tok, dm.ff, dm.slots
        group = dm.n_chip * 2 * tok

        vm = pl.BlockSpec(memory_space=pltpu.VMEM)
        sm = pl.BlockSpec(memory_space=pltpu.SMEM)
        hbm = pl.BlockSpec(memory_space=pltpu.HBM)
        dma = pltpu.SemaphoreType.DMA
        le = dm.local_e
        rows_all, pick_rows, mix, shared_act, tile_e = pl.pallas_call(
            functools.partial(gather_kernel, dm),
            out_shape=(jax.ShapeDtypeStruct((nj, dm.n_chip, 2 * tok, KC), BF16), jax.ShapeDtypeStruct((slots, group), BF16),
                       jax.ShapeDtypeStruct((group, 3 * slots), BF16), jax.ShapeDtypeStruct((tok, dm.sff), BF16),
                       jax.ShapeDtypeStruct((slots // TILE + 1,), jnp.int32)),
            in_specs=[vm] * 5 + [hbm, hbm],
            out_specs=(vm, vm, vm, vm, sm),
            scratch_shapes=[
                pltpu.VMEM((nj, tok, KC), BF16),
                pltpu.VMEM((dm.n_chip, 2, 3 * KPAD, 2 * tok), F32),
                pltpu.VMEM((dm.n_chip, 2 * tok, KPAD), F32),
                pltpu.VMEM((dm.n_chip, 2 * tok, KPAD), F32),
                pltpu.VMEM((tok, 2 * dm.sff), F32),
                pltpu.VMEM((2, 2, KC, dm.sff), BF16),
                dma((2, 2)), dma((nj,)), dma((nj,)),
                dma((hops, nj)), dma((hops, nj)), dma((hops, nj)), dma((hops, nj)),
                dma((hops,)), dma((hops,)), dma((hops,)), dma((hops,)), dma((2,)), dma((2,)),
            ],
            compiler_params=pltpu.CompilerParams(collective_id=0, has_side_effects=True, vmem_limit_bytes=36 << 20),
        )(resid_in, norm_gain.reshape(1, dm.hidden), router_w.T, expert_ids.T, priority.T, shared_w1, shared_w3)
        h_act = pl.pallas_call(
            functools.partial(up_kernel, dm),
            out_shape=jax.ShapeDtypeStruct((slots, ff), BF16),
            in_specs=[sm, vm, vm, hbm, hbm],
            out_specs=vm,
            scratch_shapes=[pltpu.VMEM((slots, dm.hidden), BF16), pltpu.VMEM((2, 2, le, dm.hidden, KC), BF16), dma((2, 2))],
            compiler_params=pltpu.CompilerParams(vmem_limit_bytes=36 << 20),
        )(tile_e, rows_all, pick_rows, expert_w1, expert_w3)
        return pl.pallas_call(
            functools.partial(down_kernel, dm),
            out_shape=jax.ShapeDtypeStruct((tok, dm.hidden), BF16),
            in_specs=[vm, vm, sm, vm, vm, hbm, hbm],
            out_specs=vm,
            scratch_shapes=[
                pltpu.VMEM((nj * group, KC), F32),
                pltpu.VMEM((le, ff, KC), BF16),
                pltpu.VMEM((le, ff, KC), BF16),
                pltpu.VMEM((dm.sff, KC), BF16),
                pltpu.VMEM((dm.sff, KC), BF16),
                pltpu.VMEM((3 * slots, KC), BF16),
                pltpu.VMEM((nj, 8 * tok, KC), F32),
                pltpu.VMEM((nj, 7 * tok, KC), F32),
                pltpu.VMEM((nj, tok, KC), F32),
                pltpu.VMEM((nj, tok, KC), BF16),
                dma((2, 2)),
                dma((hops + 1, nj)), dma((hops + 1, nj)), dma((hops, nj)), dma((hops, nj)), dma((nj,)), dma((nj,)),
            ],
            compiler_params=pltpu.CompilerParams(collective_id=1, has_side_effects=True, vmem_limit_bytes=38 << 20),
        )(h_act, mix, tile_e, shared_act, resid_in, expert_w2, shared_w2)

    return jax.shard_map(device_fn, mesh=mesh, in_specs=(tok_spec, tok_spec, tok_spec, P(), P(), P(), P(), P(), expert_spec, expert_spec, expert_spec), out_specs=tok_spec, check_vma=False)
```

```python
import functools

import jax
import jax.numpy as jnp
from jax import lax
from jax.experimental import pallas as pl
from jax.experimental.pallas import tpu as pltpu
from jax.sharding import PartitionSpec as P

NORM_EPS = 1e-6
ROUTE_SCALE = 16.0
KC = 256
TILE = 128
KPAD = 8
F32 = jnp.float32
BF16 = jnp.bfloat16


def dot(a, b):
    return jnp.dot(a, b, preferred_element_type=F32)


def ring_place(dm):
    n = dm.n_chip
    me = lax.axis_index("ep")
    chip = me // 2
    core = me - 2 * chip
    d = 1 - 2 * core

    def at(h):
        return lax.rem(chip + h * d + 2 * n, n)

    return me, chip, core, at, 2 * chip + 1 - core, 2 * at(1) + core, 2 * at(-1) + core


def rcopy(src, dst, ssem, rsem, dev):
    return pltpu.make_async_remote_copy(src_ref=src, dst_ref=dst, send_sem=ssem, recv_sem=rsem,
                                        device_id={"ep": dev}, device_id_type=pl.DeviceIdType.MESH)


def entry_signal(devs):
    barrier = pltpu.get_barrier_semaphore()
    for dev in devs:
        pl.semaphore_signal(barrier, inc=1, device_id={"ep": dev}, device_id_type=pl.DeviceIdType.MESH)


def entry_wait(count):
    pl.semaphore_wait(pltpu.get_barrier_semaphore(), count)


def entry_barrier(devs):
    entry_signal(devs)
    entry_wait(len(devs))


def cond(static, pred, fn):
    if static:
        if pred:
            fn()
    else:
        pl.when(pred)(fn)


def start(copies):
    for c in copies:
        c.start()


def wait(copies):
    for c in copies:
        c.wait()


def gather_kernel(dm, rows_ref, small_ref, sw1, sw3, X, PG, WC, HS, TE,
                  B, I, SLT, GLT, SACC, WS, wsem, xs_other, xr_other, xs_ring, xr_ring, xs_d2d, xr_d2d, is_ring, ir_ring, is_d2d, ir_d2d, p_s, p_r):
    n = dm.n_chip
    hops = n // 2
    tok = dm.tok
    crows = 2 * tok
    nj = dm.nj
    slots = dm.slots
    n_tiles = slots // TILE
    group = n * crows
    me, chip, core, at, partner, down, up = ring_place(dm)
    half = pl.ds(pl.multiple_of(core * tok, tok), tok)
    sff = dm.sff

    def shared_copies(t):
        rows = pl.ds(t * KC, KC)
        return [pltpu.make_async_copy(src.at[rows, :], WS.at[t % 2, m], wsem.at[t % 2, m]) for m, src in enumerate((sw1, sw3))]

    def shared_stage(t):
        wait(shared_copies(t))
        x = B[t]
        for m in range(2):
            for c in range(sff // KC):
                dst = pl.ds(m * sff + c * KC, KC)
                val = dot(x, WS[t % 2, m, :, pl.ds(c * KC, KC)])
                if t == 0:
                    SACC[:, dst] = val
                else:
                    SACC[:, dst] += val
        if t + 2 < nj:
            start(shared_copies(t + 2))

    entry_signal((partner, down, up))
    for t in range(2):
        start(shared_copies(t))

    resid32 = rows_ref[pl.ds(0, tok), :].astype(F32)
    inv_rms = lax.rsqrt(jnp.mean(resid32 * resid32, axis=1, keepdims=True) + NORM_EPS)
    normed = (resid32 * inv_rms * small_ref[pl.ds(0, 1), :]).astype(BF16)
    for j in range(nj):
        B[j] = normed[:, j * KC:(j + 1) * KC]
        X[j, chip, half, :] = normed[:, j * KC:(j + 1) * KC]
    logits = lax.dot_general(rows_ref[pl.ds(tok, rows_ref.shape[0] - tok), :], normed, (((1,), (1,)), ((), ())), preferred_element_type=F32)
    powers = jnp.exp(logits - jnp.max(logits, axis=0, keepdims=True))
    probs = powers / jnp.sum(powers, axis=0, keepdims=True)
    experts = lax.broadcasted_iota(jnp.int32, probs.shape, 0).astype(F32)
    ids = small_ref[pl.ds(1, dm.top_k), pl.ds(0, tok)]
    prio_in = small_ref[pl.ds(1 + dm.top_k, dm.top_k), pl.ds(0, tok)]

    def put(i, k, row):
        zero = jnp.zeros((1, tok), F32)
        I[chip, core, pl.ds(i * KPAD + k, 1), :] = jnp.where(core == 0, jnp.concatenate([row, zero], axis=1), jnp.concatenate([zero, row], axis=1))

    for k in range(KPAD):
        if k < dm.top_k:
            put(0, k, ids[k:k + 1])
            put(1, k, prio_in[k:k + 1])
            put(2, k, ROUTE_SCALE * jnp.sum(jnp.where(experts == ids[k:k + 1], probs, 0.0), axis=0, keepdims=True))
        else:
            put(0, k, jnp.full((1, tok), -1.0, F32))
            put(1, k, jnp.zeros((1, tok), F32))
            put(2, k, jnp.zeros((1, tok), F32))

    entry_wait(3)
    own_x = X.at[:, chip, half, :]
    own_i = I.at[chip, core]
    first = [rcopy(own_i, own_i, p_s.at[1], p_r.at[1], partner), rcopy(own_x, own_x, p_s.at[0], p_r.at[0], partner)]
    start(first)

    def x_block(j, h, rows_half):
        return X.at[j, at(-h), half, :] if rows_half else X.at[j, at(-h)]

    def x_ring(j, h):
        blk = x_block(j, h, h + 1 == hops)
        return rcopy(blk, blk, xs_ring.at[h, j], xr_ring.at[h, j], down)

    def x_ring_in(j, h):
        blk = x_block(j, h, h == hops)
        return rcopy(blk, blk, xs_ring.at[h - 1, j], xr_ring.at[h - 1, j], down)

    def x_d2d(j, h):
        blk = x_block(j, h, h == hops)
        return rcopy(blk, blk, xs_d2d.at[h - 1, j], xr_d2d.at[h - 1, j], partner)

    def x_d2d_in(j, h):
        blk = X.at[j, at(h), pl.ds(pl.multiple_of((1 - core) * tok, tok), tok), :] if h == hops else X.at[j, at(h)]
        return rcopy(blk, blk, xs_d2d.at[h - 1, j], xr_d2d.at[h - 1, j], partner)

    def x_part(j, h, other):
        rows = pl.ds(pl.multiple_of((1 - core) * tok, tok), tok) if other else half
        blk = X.at[j, at(-h), rows, :]
        return rcopy(blk, blk, xs_other.at[j], xr_other.at[j], down) if other else rcopy(blk, blk, xs_ring.at[0, j], xr_ring.at[0, j], down)

    def forward(h, j):
        if h == 1:
            x_part(j, 1, False).wait_recv()
            x_part(j, 1, True).wait_recv()
        elif h > 1:
            x_ring_in(j, h).wait_recv()
        if h < hops:
            x_ring(j, h).start()
        if h > 0:
            x_d2d(j, h).start()

    def i_block(h, rows_half, sign=-1, c=None):
        return I.at[at(sign * h), core if c is None else c] if rows_half else I.at[at(sign * h)]

    def comm_info(h):
        if h > 0:
            blk = i_block(h, h == hops)
            rcopy(blk, blk, is_ring.at[h - 1], ir_ring.at[h - 1], down).wait_recv()
        if h < hops:
            blk = i_block(h, h + 1 == hops)
            rcopy(blk, blk, is_ring.at[h], ir_ring.at[h], down).start()
        if h > 0:
            blk = i_block(h, h == hops)
            rcopy(blk, blk, is_d2d.at[h - 1], ir_d2d.at[h - 1], partner).start()

    for j in range(nj // 2):
        x_part(j, 0, False).start()
    first[0].wait_recv()
    comm_info(0)
    for j in range(nj // 2, nj):
        x_part(j, 0, False).start()
    first[1].wait_recv()
    for j in range(nj // 2):
        x_part(j, 0, True).start()
    comm_info(1)
    for j in range(nj // 2, nj):
        x_part(j, 0, True).start()
    shared_stage(0)
    shared_stage(1)
    for j in range(3):
        forward(1, j)
    comm_info(2)
    shared_stage(2)
    for j in range(3, 6):
        forward(1, j)
    shared_stage(3)
    for j in range(6, 8):
        forward(1, j)
    comm_info(3)
    shared_stage(4)
    for j in range(8, nj):
        forward(1, j)
    shared_stage(5)
    for j in range(2):
        forward(2, j)
    comm_info(hops)
    for j in range(2, 4):
        forward(2, j)

    for h in range(1, hops + 1):
        blk = i_block(h, h == hops, 1, 1 - core)
        rcopy(blk, blk, is_d2d.at[h - 1], ir_d2d.at[h - 1], partner).wait_recv()

    lanes = crows
    nr = n * KPAD

    def field(i):
        rows = pl.ds(i * KPAD, KPAD)
        return (I[:, 0, rows, :] + I[:, 1, rows, :]).reshape(nr, lanes)

    mine_e = field(0) - (me * dm.local_e).astype(F32)
    prio = field(1)
    gate = field(2)
    mine = (mine_e >= 0) & (mine_e < dm.local_e)
    key = jnp.where(mine, prio, 1e9)
    cut = jnp.zeros((1, 1), F32)
    bit = 1 << (group * dm.top_k).bit_length()
    while bit >= 1:
        cand = cut + float(bit)
        cnt = jnp.sum(jnp.where(key < cand, 1.0, 0.0), keepdims=True)
        cut = jnp.where(cnt <= float(dm.capacity), cand, cut)
        bit //= 2
    kept = key < cut
    masks = [jnp.where(kept & (mine_e == float(e)), 1.0, 0.0) for e in range(dm.local_e)]
    stack = jnp.concatenate(masks, axis=0)
    li = lax.broadcasted_iota(jnp.int32, (lanes, lanes), 0)
    lj = lax.broadcasted_iota(jnp.int32, (lanes, lanes), 1)
    upper = jnp.where(li <= lj, 1.0, 0.0).astype(BF16)
    inrow = dot(stack.astype(BF16), upper)
    total_rows = dm.local_e * nr
    rowtot = jnp.broadcast_to(inrow[:, lanes - 1:lanes], (total_rows, lanes))
    ri = lax.broadcasted_iota(jnp.int32, (total_rows, total_rows), 0)
    rj = lax.broadcasted_iota(jnp.int32, (total_rows, total_rows), 1)
    lower = jnp.where((ri > rj) & (ri // nr == rj // nr), 1.0, 0.0).astype(BF16)
    before = dot(lower, rowtot.astype(BF16))
    slot_of = jnp.full((nr, lanes), -1.0, F32)
    base = jnp.zeros((1, lanes), F32)
    bound = jnp.int32(0)
    bounds = []
    for e in range(dm.local_e):
        rows = slice(e * nr, (e + 1) * nr)
        pos = base + before[rows] + inrow[rows] - 1.0
        slot_of = jnp.where(masks[e] > 0.5, pos, slot_of)
        last = (e + 1) * nr - 1
        count = before[last:last + 1] + rowtot[last:last + 1]
        base = base + jnp.floor((count + (TILE - 1.0)) * (1.0 / TILE)) * TILE
        count_i = jnp.sum(jnp.where(kept & (mine_e == float(e)), 1, 0))
        bound = bound + (count_i + (TILE - 1)) // TILE
        bounds.append(bound)
    tile_e = [sum(jnp.where(bounds[e] <= i, 1, 0) for e in range(dm.local_e - 1)) for i in range(n_tiles)]

    slot_t = slot_of.T
    gate_t = gate.T
    for c in range(n):
        SLT[c] = slot_t[:, c * KPAD:(c + 1) * KPAD]
        GLT[c] = gate_t[:, c * KPAD:(c + 1) * KPAD]

    for i in range(n_tiles):
        TE[i] = tile_e[i]
    TE[n_tiles] = bounds[dm.local_e - 1]

    def pick_rows(c):
        for r in range(n_tiles):
            srow = (lax.broadcasted_iota(jnp.int32, (TILE, lanes), 0) + r * TILE).astype(F32)
            hit = jnp.zeros((TILE, lanes), F32)
            for k in range(dm.top_k):
                hit = jnp.where(slot_of[c * KPAD + k:c * KPAD + k + 1] == srow, 1.0, hit)
            PG[pl.ds(r * TILE, TILE), pl.ds(c * lanes, lanes)] = hit.astype(BF16)

    def combine_rows(c):
        sl = SLT[c]
        gl = GLT[c]
        rows = pl.ds(c * crows, crows)
        for p in range(slots // KC):
            scol = (lax.broadcasted_iota(jnp.int32, (crows, KC), 1) + p * KC).astype(F32)
            w = jnp.zeros((crows, KC), F32)
            for k in range(dm.top_k):
                w = jnp.where(sl[:, k:k + 1] == scol, gl[:, k:k + 1], w)
            for i in range(3):
                part = w.astype(BF16)
                WC[rows, pl.ds(i * slots + p * KC, KC)] = part
                w = w - part.astype(F32)

    todo = [(2, j) for j in range(4, nj)] + [(3, j) for j in range(nj)]
    work = []
    for t in range(n):
        work.append(functools.partial(pick_rows, t))
        if t < nj - 6:
            work.append(functools.partial(shared_stage, t + 6))
        work.append(functools.partial(combine_rows, t))
    total = len(work)
    for u, (h, j) in enumerate(todo):
        forward(h, j)
        while len(work) > total * (len(todo) - 1 - u) // len(todo):
            work.pop(0)()
    for c in range(sff // KC):
        a = SACC[:, pl.ds(c * KC, KC)]
        g = SACC[:, pl.ds(sff + c * KC, KC)]
        HS[:, pl.ds(c * KC, KC)] = (jax.nn.silu(a) * g).astype(BF16)

    def last_hop(j, carry):
        forward(hops, j)
        return carry

    lax.fori_loop(0, nj, last_hop, 0)

    def arrive(j, carry):
        for h in range(1, hops + 1):
            x_d2d_in(j, h).wait_recv()
        return carry

    lax.fori_loop(0, nj, arrive, 0)
    for c in first:
        c.wait_send()
    for h in range(hops):
        blk = i_block(h, h + 1 == hops)
        rcopy(blk, blk, is_ring.at[h], ir_ring.at[h], down).wait_send()
        blk = i_block(h + 1, h + 1 == hops)
        rcopy(blk, blk, is_d2d.at[h], ir_d2d.at[h], partner).wait_send()

    def drain(j, carry):
        x_part(j, 0, False).wait_send()
        x_part(j, 0, True).wait_send()
        for h in range(hops):
            if h > 0:
                x_ring(j, h).wait_send()
            x_d2d(j, h + 1).wait_send()
        return carry

    lax.fori_loop(0, nj, drain, 0)


def up_kernel(dm, te_ref, x_ref, pg_ref, w1, w3, h_ref, xg_ref, w_ref, wsem):
    n_tiles = dm.slots // TILE
    nt = dm.ff // KC

    def copies(c, slot):
        cols = pl.ds(pl.multiple_of(c * KC, KC), KC)
        return [pltpu.make_async_copy(src.at[:, :, cols], w_ref.at[slot, m], wsem.at[slot, m]) for m, src in enumerate((w1, w3))]

    depth = w_ref.shape[0]
    for c in range(depth):
        start(copies(c, c))

    def pick(j, carry):
        xg_ref[:, pl.ds(pl.multiple_of(j * KC, KC), KC)] = dot(pg_ref[...], x_ref[j].reshape(pg_ref.shape[1], KC)).astype(BF16)
        return carry

    lax.fori_loop(0, dm.nj, pick, 0)

    def column(c, carry):
        slot = c % depth
        cols = pl.ds(pl.multiple_of(c * KC, KC), KC)
        wait(copies(c, slot))
        for i in range(n_tiles):
            rows = pl.ds(i * TILE, TILE)

            @pl.when(i < te_ref[n_tiles])
            def _():
                e = te_ref[i]
                a = dot(xg_ref[rows, :], w_ref[slot, 0, e])
                g = dot(xg_ref[rows, :], w_ref[slot, 1, e])
                h_ref[rows, cols] = (jax.nn.silu(a) * g).astype(BF16)

            @pl.when(i >= te_ref[n_tiles])
            def _():
                h_ref[rows, cols] = jnp.zeros((TILE, KC), BF16)

        @pl.when(c + depth < nt)
        def _():
            start(copies(c + depth, slot))
        return carry

    lax.fori_loop(0, nt, column, 0)


def down_kernel(dm, H, WC, TE, HS, resid_ref, ew2, sw2, out_ref,
                BIG, V2A, V2B, S2A, S2B, E3, PR, RR, FR, SOUT, vsem, qs, qr, rs, rr, fs, fr):
    n = dm.n_chip
    hops = n // 2
    tok = dm.tok
    crows = 2 * tok
    nj = dm.nj
    slots = dm.slots
    n_tiles = slots // TILE
    group = n * crows
    me, chip, core, at, partner, down, up = ring_place(dm)
    V2 = (V2A, V2B)
    S2 = (S2A, S2B)

    def down_copies(j, slot):
        cols = pl.ds(pl.multiple_of(j * KC, KC), KC)
        return [pltpu.make_async_copy(ew2.at[:, :, cols], V2[slot], vsem.at[slot, 0])]

    def shared_copies(j, slot):
        cols = pl.ds(pl.multiple_of(j * KC, KC), KC)
        return [pltpu.make_async_copy(sw2.at[:, cols], S2[slot], vsem.at[slot, 1])]

    def shared_step(j, slot, more):
        wait(shared_copies(j, slot))
        SOUT[j] = dot(HS[...], S2[slot][...]).astype(BF16)
        if more:
            start(shared_copies(j + 2, slot))

    start(down_copies(0, 0))
    start(down_copies(1, 1))
    start(shared_copies(0, 0))
    start(shared_copies(1, 1))
    entry_barrier((partner, down, up))

    pr_off = [448, 0, 128, 256, 384]
    assert crows == 128 and hops == 4

    def dblk(j, dest, row, size):
        return pl.ds(pl.multiple_of(j * group + dest * crows + row, tok), size)

    def q_copy(j, h):
        if h == 0:
            src, size = BIG.at[dblk(j, chip, (1 - core) * tok, tok), :], tok
        elif h == hops:
            src, size = BIG.at[dblk(j, at(-h), (1 - core) * tok, tok), :], tok
        else:
            src, size = BIG.at[dblk(j, at(-h), 0, crows), :], crows
        return rcopy(src, PR.at[j, pl.ds(pr_off[h], size), :], qs.at[h, j], qr.at[h, j], partner)

    rr_off = [0, 64, 192, 320]

    def r_copy(j, g):
        h = hops - g
        src, size = (BIG.at[dblk(j, at(h), core * tok, tok), :], tok) if g == 0 else (BIG.at[dblk(j, at(h), 0, crows), :], crows)
        return rcopy(src, RR.at[j, pl.ds(rr_off[g], size), :], rs.at[g, j], rr.at[g, j], down)

    def f_copy(j):
        return rcopy(RR.at[j, pl.ds(pl.multiple_of(rr_off[hops - 1] + (1 - core) * tok, tok), tok), :], FR.at[j], fs.at[j], fr.at[j], partner)

    def finish(j):
        q_copy(j, 0).wait_recv()
        f_copy(j).wait_recv()
        cols = pl.ds(pl.multiple_of(j * KC, KC), KC)
        routed = BIG[dblk(j, chip, core * tok, tok), :] + PR[j, pl.ds(pr_off[0], tok), :]
        routed = routed + RR[j, pl.ds(pl.multiple_of(rr_off[hops - 1] + core * tok, tok), tok), :] + FR[j]
        out_ref[:, cols] = (resid_ref[:, cols].astype(F32) + SOUT[j].astype(F32) + routed).astype(BF16)

    def turn(j):
        r_copy(j, hops - 1).wait_recv()
        f_copy(j).start()

    def relay(j, g):
        h = hops - g
        q_copy(j, h).wait_recv()
        if g == 0:
            rows = dblk(j, at(h), core * tok, tok)
            BIG[rows, :] += PR[j, pl.ds(pr_off[h], tok), :]
        else:
            r_copy(j, g - 1).wait_recv()
            rows = dblk(j, at(h), 0, crows)
            if g == 1:
                BIG[rows, :] += PR[j, pl.ds(pr_off[h], crows), :]
                hrows = dblk(j, at(h), core * tok, tok)
                BIG[hrows, :] += RR[j, pl.ds(rr_off[0], tok), :]
            else:
                BIG[rows, :] += PR[j, pl.ds(pr_off[h], crows), :] + RR[j, pl.ds(rr_off[g - 1], crows), :]
        r_copy(j, g).start()

    skew = 2
    late = nj // 2

    def ring(s, static):
        def ok(j):
            return (0 <= j < nj) if static else (j >= 0)
        for g in range(hops):
            j = s - skew * (g + 1)
            cond(static, ok(j), functools.partial(relay, j, g))
        j = s - skew * (hops + 1)
        cond(static, ok(j), functools.partial(turn, j))
        cond(static, ok(j - 1), functools.partial(finish, j - 1))

    def down_step(j, slot):
        ring(j, False)
        wait(down_copies(j, slot))
        for i in range(n_tiles):
            e = dot(H[pl.ds(i * TILE, TILE), :], V2[slot][TE[i]]).astype(BF16)
            for p in range(3):
                E3[pl.ds(p * slots + i * TILE, TILE), :] = e
        for r in range(group // KC):
            rows = pl.ds(pl.multiple_of(j * group + r * KC, KC), KC)
            BIG[rows, :] = dot(WC[pl.ds(r * KC, KC), :], E3[...])
        for h in range(hops, -1, -1):
            q_copy(j, h).start()

        @pl.when(j + 2 < nj)
        def _():
            start(down_copies(j + 2, slot))

        @pl.when(j >= late)
        def _():
            shared_step(j - late, (slot + late) % 2, True)

    def down_pair(p, carry):
        for q in range(2):
            down_step(2 * p + q, q)
        return carry

    lax.fori_loop(0, nj // 2, down_pair, 0)
    for s in range(nj, nj + skew * (hops + 1) + 1):
        ring(s, True)
        if 0 <= s - late < nj:
            shared_step(s - late, (s - late) % 2, s - late + 2 < nj)

    def drain(j, carry):
        for h in range(hops):
            r_copy(j, h).wait_send()
        for h in range(hops + 1):
            q_copy(j, h).wait_send()
        f_copy(j).wait_send()
        return carry

    lax.fori_loop(0, nj, drain, 0)


class Dims:
    pass


def solution(mesh):
    n_ep = mesh.shape['ep']
    tok_spec = P(('dp', 'ep'))
    expert_spec = P('ep')

    def device_fn(resid_in, expert_ids, priority, norm_gain, router_w, shared_w1, shared_w3, shared_w2, expert_w1, expert_w3, expert_w2):
        dm = Dims()
        dm.n_chip = n_ep // 2
        dm.tok, dm.hidden = resid_in.shape
        dm.top_k = expert_ids.shape[1]
        dm.local_e = expert_w1.shape[0]
        dm.ff = expert_w1.shape[2]
        dm.capacity = dm.tok * dm.top_k
        dm.nj = dm.hidden // KC
        dm.sff = shared_w1.shape[1]
        dm.slots = (dm.capacity + dm.local_e * (TILE - 1)) // TILE * TILE
        hops = dm.n_chip // 2
        assert dm.nj % 2 == 0
        nj, tok, ff, slots = dm.nj, dm.tok, dm.ff, dm.slots
        group = dm.n_chip * 2 * tok

        vm = pl.BlockSpec(memory_space=pltpu.VMEM)
        sm = pl.BlockSpec(memory_space=pltpu.SMEM)
        hbm = pl.BlockSpec(memory_space=pltpu.HBM)
        dma = pltpu.SemaphoreType.DMA
        le = dm.local_e
        rows_in = jnp.concatenate([resid_in, router_w.T], axis=0)

        def wide(a):
            return jnp.pad(a.T.astype(F32), ((0, 0), (0, dm.hidden - tok)))

        small_in = jnp.concatenate([norm_gain.reshape(1, dm.hidden), wide(expert_ids), wide(priority)], axis=0)
        rows_all, pick_rows, mix, shared_act, tile_e = pl.pallas_call(
            functools.partial(gather_kernel, dm),
            out_shape=(jax.ShapeDtypeStruct((nj, dm.n_chip, 2 * tok, KC), BF16), jax.ShapeDtypeStruct((slots, group), BF16),
                       jax.ShapeDtypeStruct((group, 3 * slots), BF16), jax.ShapeDtypeStruct((tok, dm.sff), BF16),
                       jax.ShapeDtypeStruct((slots // TILE + 1,), jnp.int32)),
            in_specs=[vm, vm, hbm, hbm],
            out_specs=(vm, vm, vm, vm, sm),
            scratch_shapes=[
                pltpu.VMEM((nj, tok, KC), BF16),
                pltpu.VMEM((dm.n_chip, 2, 3 * KPAD, 2 * tok), F32),
                pltpu.VMEM((dm.n_chip, 2 * tok, KPAD), F32),
                pltpu.VMEM((dm.n_chip, 2 * tok, KPAD), F32),
                pltpu.VMEM((tok, 2 * dm.sff), F32),
                pltpu.VMEM((2, 2, KC, dm.sff), BF16),
                dma((2, 2)), dma((nj,)), dma((nj,)),
                dma((hops, nj)), dma((hops, nj)), dma((hops, nj)), dma((hops, nj)),
                dma((hops,)), dma((hops,)), dma((hops,)), dma((hops,)), dma((2,)), dma((2,)),
            ],
            compiler_params=pltpu.CompilerParams(collective_id=0, has_side_effects=True, vmem_limit_bytes=36 << 20),
        )(rows_in, small_in, shared_w1, shared_w3)
        h_act = pl.pallas_call(
            functools.partial(up_kernel, dm),
            out_shape=jax.ShapeDtypeStruct((slots, ff), BF16),
            in_specs=[sm, vm, vm, hbm, hbm],
            out_specs=vm,
            scratch_shapes=[pltpu.VMEM((slots, dm.hidden), BF16), pltpu.VMEM((3, 2, le, dm.hidden, KC), BF16), dma((3, 2))],
            compiler_params=pltpu.CompilerParams(vmem_limit_bytes=40 << 20),
        )(tile_e, rows_all, pick_rows, expert_w1, expert_w3)
        return pl.pallas_call(
            functools.partial(down_kernel, dm),
            out_shape=jax.ShapeDtypeStruct((tok, dm.hidden), BF16),
            in_specs=[vm, vm, sm, vm, vm, hbm, hbm],
            out_specs=vm,
            scratch_shapes=[
                pltpu.VMEM((nj * group, KC), F32),
                pltpu.VMEM((le, ff, KC), BF16),
                pltpu.VMEM((le, ff, KC), BF16),
                pltpu.VMEM((dm.sff, KC), BF16),
                pltpu.VMEM((dm.sff, KC), BF16),
                pltpu.VMEM((3 * slots, KC), BF16),
                pltpu.VMEM((nj, 8 * tok, KC), F32),
                pltpu.VMEM((nj, 7 * tok, KC), F32),
                pltpu.VMEM((nj, tok, KC), F32),
                pltpu.VMEM((nj, tok, KC), BF16),
                dma((2, 2)),
                dma((hops + 1, nj)), dma((hops + 1, nj)), dma((hops, nj)), dma((hops, nj)), dma((nj,)), dma((nj,)),
            ],
            compiler_params=pltpu.CompilerParams(collective_id=1, has_side_effects=True, vmem_limit_bytes=38 << 20),
        )(h_act, mix, tile_e, shared_act, resid_in, expert_w2, shared_w2)

    return jax.shard_map(device_fn, mesh=mesh, in_specs=(tok_spec, tok_spec, tok_spec, P(), P(), P(), P(), P(), expert_spec, expert_spec, expert_spec), out_specs=tok_spec, check_vma=False)
```

```python
import functools

import jax
import jax.numpy as jnp
from jax import lax
from jax.experimental import pallas as pl
from jax.experimental.pallas import tpu as pltpu
from jax.sharding import PartitionSpec as P

NORM_EPS = 1e-6
ROUTE_SCALE = 16.0
KC = 256
TILE = 128
KPAD = 8
F32 = jnp.float32
BF16 = jnp.bfloat16


def dot(a, b):
    return jnp.dot(a, b, preferred_element_type=F32)


def ring_place(dm):
    n = dm.n_chip
    me = lax.axis_index("ep")
    chip = me // 2
    core = me - 2 * chip
    d = 1 - 2 * core

    def at(h):
        return lax.rem(chip + h * d + 2 * n, n)

    return me, chip, core, at, 2 * chip + 1 - core, 2 * at(1) + core, 2 * at(-1) + core


def rcopy(src, dst, ssem, rsem, dev):
    return pltpu.make_async_remote_copy(src_ref=src, dst_ref=dst, send_sem=ssem, recv_sem=rsem,
                                        device_id={"ep": dev}, device_id_type=pl.DeviceIdType.MESH)


def entry_signal(devs):
    barrier = pltpu.get_barrier_semaphore()
    for dev in devs:
        pl.semaphore_signal(barrier, inc=1, device_id={"ep": dev}, device_id_type=pl.DeviceIdType.MESH)


def entry_wait(count):
    pl.semaphore_wait(pltpu.get_barrier_semaphore(), count)


def entry_barrier(devs):
    entry_signal(devs)
    entry_wait(len(devs))


def cond(static, pred, fn):
    if static:
        if pred:
            fn()
    else:
        pl.when(pred)(fn)


def start(copies):
    for c in copies:
        c.start()


def wait(copies):
    for c in copies:
        c.wait()


def gather_kernel(dm, rows_ref, small_ref, sw1, sw3, X, PG, WC, HS, TE,
                  B, I, SLT, GLT, SACC, WS, wsem, xs_other, xr_other, xs_ring, xr_ring, xs_d2d, xr_d2d, is_ring, ir_ring, is_d2d, ir_d2d, p_s, p_r):
    n = dm.n_chip
    hops = n // 2
    tok = dm.tok
    crows = 2 * tok
    nj = dm.nj
    slots = dm.slots
    n_tiles = slots // TILE
    group = n * crows
    me, chip, core, at, partner, down, up = ring_place(dm)
    half = pl.ds(pl.multiple_of(core * tok, tok), tok)
    sff = dm.sff

    def shared_copies(t):
        rows = pl.ds(t * KC, KC)
        return [pltpu.make_async_copy(src.at[rows, :], WS.at[t % 2, m], wsem.at[t % 2, m]) for m, src in enumerate((sw1, sw3))]

    def shared_stage(t):
        wait(shared_copies(t))
        x = B[t]
        for m in range(2):
            for c in range(sff // KC):
                dst = pl.ds(m * sff + c * KC, KC)
                val = dot(x, WS[t % 2, m, :, pl.ds(c * KC, KC)])
                if t == 0:
                    SACC[:, dst] = val
                else:
                    SACC[:, dst] += val
        if t + 2 < nj:
            start(shared_copies(t + 2))

    entry_signal((partner, down, up))
    for t in range(2):
        start(shared_copies(t))

    resid32 = rows_ref[pl.ds(0, tok), :].astype(F32)
    inv_rms = lax.rsqrt(jnp.mean(resid32 * resid32, axis=1, keepdims=True) + NORM_EPS)
    normed = (resid32 * inv_rms * small_ref[pl.ds(0, 1), :]).astype(BF16)
    for j in range(nj):
        B[j] = normed[:, j * KC:(j + 1) * KC]
        X[j, chip, half, :] = normed[:, j * KC:(j + 1) * KC]
    logits = lax.dot_general(rows_ref[pl.ds(tok, rows_ref.shape[0] - tok), :], normed, (((1,), (1,)), ((), ())), preferred_element_type=F32)
    powers = jnp.exp(logits - jnp.max(logits, axis=0, keepdims=True))
    probs = powers / jnp.sum(powers, axis=0, keepdims=True)
    experts = lax.broadcasted_iota(jnp.int32, probs.shape, 0).astype(F32)
    ids = small_ref[pl.ds(1, dm.top_k), pl.ds(0, tok)]
    prio_in = small_ref[pl.ds(1 + dm.top_k, dm.top_k), pl.ds(0, tok)]

    def put(i, k, row):
        zero = jnp.zeros((1, tok), F32)
        I[chip, core, pl.ds(i * KPAD + k, 1), :] = jnp.where(core == 0, jnp.concatenate([row, zero], axis=1), jnp.concatenate([zero, row], axis=1))

    for k in range(KPAD):
        if k < dm.top_k:
            put(0, k, ids[k:k + 1])
            put(1, k, prio_in[k:k + 1])
            put(2, k, ROUTE_SCALE * jnp.sum(jnp.where(experts == ids[k:k + 1], probs, 0.0), axis=0, keepdims=True))
        else:
            put(0, k, jnp.full((1, tok), -1.0, F32))
            put(1, k, jnp.zeros((1, tok), F32))
            put(2, k, jnp.zeros((1, tok), F32))

    entry_wait(3)
    own_x = X.at[:, chip, half, :]
    own_i = I.at[chip, core]
    first = [rcopy(own_i, own_i, p_s.at[1], p_r.at[1], partner), rcopy(own_x, own_x, p_s.at[0], p_r.at[0], partner)]
    start(first)

    def x_block(j, h, rows_half):
        return X.at[j, at(-h), half, :] if rows_half else X.at[j, at(-h)]

    def x_ring(j, h):
        blk = x_block(j, h, h + 1 == hops)
        return rcopy(blk, blk, xs_ring.at[h, j], xr_ring.at[h, j], down)

    def x_ring_in(j, h):
        blk = x_block(j, h, h == hops)
        return rcopy(blk, blk, xs_ring.at[h - 1, j], xr_ring.at[h - 1, j], down)

    def x_d2d(j, h):
        blk = x_block(j, h, h == hops)
        return rcopy(blk, blk, xs_d2d.at[h - 1, j], xr_d2d.at[h - 1, j], partner)

    def x_d2d_in(j, h):
        blk = X.at[j, at(h), pl.ds(pl.multiple_of((1 - core) * tok, tok), tok), :] if h == hops else X.at[j, at(h)]
        return rcopy(blk, blk, xs_d2d.at[h - 1, j], xr_d2d.at[h - 1, j], partner)

    def x_part(j, h, other):
        rows = pl.ds(pl.multiple_of((1 - core) * tok, tok), tok) if other else half
        blk = X.at[j, at(-h), rows, :]
        return rcopy(blk, blk, xs_other.at[j], xr_other.at[j], down) if other else rcopy(blk, blk, xs_ring.at[0, j], xr_ring.at[0, j], down)

    def forward(h, j):
        if h == 1:
            x_part(j, 1, False).wait_recv()
            x_part(j, 1, True).wait_recv()
        elif h > 1:
            x_ring_in(j, h).wait_recv()
        if h < hops:
            x_ring(j, h).start()
        if h > 0:
            x_d2d(j, h).start()

    def i_block(h, rows_half, sign=-1, c=None):
        return I.at[at(sign * h), core if c is None else c] if rows_half else I.at[at(sign * h)]

    def comm_info(h):
        if h > 0:
            blk = i_block(h, h == hops)
            rcopy(blk, blk, is_ring.at[h - 1], ir_ring.at[h - 1], down).wait_recv()
        if h < hops:
            blk = i_block(h, h + 1 == hops)
            rcopy(blk, blk, is_ring.at[h], ir_ring.at[h], down).start()
        if h > 0:
            blk = i_block(h, h == hops)
            rcopy(blk, blk, is_d2d.at[h - 1], ir_d2d.at[h - 1], partner).start()

    for j in range(nj // 2):
        x_part(j, 0, False).start()
    first[0].wait_recv()
    comm_info(0)
    for j in range(nj // 2, nj):
        x_part(j, 0, False).start()
    first[1].wait_recv()
    for j in range(nj // 2):
        x_part(j, 0, True).start()
    comm_info(1)
    for j in range(nj // 2, nj):
        x_part(j, 0, True).start()
    shared_stage(0)
    shared_stage(1)
    for j in range(3):
        forward(1, j)
    comm_info(2)
    shared_stage(2)
    for j in range(3, 6):
        forward(1, j)
    shared_stage(3)
    for j in range(6, 8):
        forward(1, j)
    comm_info(3)
    shared_stage(4)
    for j in range(8, nj):
        forward(1, j)
    shared_stage(5)
    for j in range(2):
        forward(2, j)
    comm_info(hops)
    for j in range(2, 4):
        forward(2, j)

    for h in range(1, hops + 1):
        blk = i_block(h, h == hops, 1, 1 - core)
        rcopy(blk, blk, is_d2d.at[h - 1], ir_d2d.at[h - 1], partner).wait_recv()

    lanes = crows
    nr = n * KPAD

    def field(i):
        rows = pl.ds(i * KPAD, KPAD)
        return (I[:, 0, rows, :] + I[:, 1, rows, :]).reshape(nr, lanes)

    mine_e = field(0) - (me * dm.local_e).astype(F32)
    prio = field(1)
    gate = field(2)
    mine = (mine_e >= 0) & (mine_e < dm.local_e)
    key = jnp.where(mine, prio, 1e9)
    cut = jnp.zeros((1, 1), F32)
    bit = 1 << (group * dm.top_k).bit_length()
    while bit >= 1:
        cand = cut + float(bit)
        cnt = jnp.sum(jnp.where(key < cand, 1.0, 0.0), keepdims=True)
        cut = jnp.where(cnt <= float(dm.capacity), cand, cut)
        bit //= 2
    kept = key < cut
    masks = [jnp.where(kept & (mine_e == float(e)), 1.0, 0.0) for e in range(dm.local_e)]
    stack = jnp.concatenate(masks, axis=0)
    li = lax.broadcasted_iota(jnp.int32, (lanes, lanes), 0)
    lj = lax.broadcasted_iota(jnp.int32, (lanes, lanes), 1)
    upper = jnp.where(li <= lj, 1.0, 0.0).astype(BF16)
    inrow = dot(stack.astype(BF16), upper)
    total_rows = dm.local_e * nr
    rowtot = jnp.broadcast_to(inrow[:, lanes - 1:lanes], (total_rows, lanes))
    ri = lax.broadcasted_iota(jnp.int32, (total_rows, total_rows), 0)
    rj = lax.broadcasted_iota(jnp.int32, (total_rows, total_rows), 1)
    lower = jnp.where((ri > rj) & (ri // nr == rj // nr), 1.0, 0.0).astype(BF16)
    before = dot(lower, rowtot.astype(BF16))
    slot_of = jnp.full((nr, lanes), -1.0, F32)
    base = jnp.zeros((1, lanes), F32)
    bound = jnp.int32(0)
    bounds = []
    for e in range(dm.local_e):
        rows = slice(e * nr, (e + 1) * nr)
        pos = base + before[rows] + inrow[rows] - 1.0
        slot_of = jnp.where(masks[e] > 0.5, pos, slot_of)
        last = (e + 1) * nr - 1
        count = before[last:last + 1] + rowtot[last:last + 1]
        base = base + jnp.floor((count + (TILE - 1.0)) * (1.0 / TILE)) * TILE
        count_i = jnp.sum(jnp.where(kept & (mine_e == float(e)), 1, 0))
        bound = bound + (count_i + (TILE - 1)) // TILE
        bounds.append(bound)
    tile_e = [sum(jnp.where(bounds[e] <= i, 1, 0) for e in range(dm.local_e - 1)) for i in range(n_tiles)]

    slot_t = slot_of.T
    gate_t = gate.T
    for c in range(n):
        SLT[c] = slot_t[:, c * KPAD:(c + 1) * KPAD]
        GLT[c] = gate_t[:, c * KPAD:(c + 1) * KPAD]

    for i in range(n_tiles):
        TE[i] = tile_e[i]
    TE[n_tiles] = bounds[dm.local_e - 1]

    def pick_rows(c):
        for r in range(n_tiles):
            srow = (lax.broadcasted_iota(jnp.int32, (TILE, lanes), 0) + r * TILE).astype(F32)
            hit = jnp.zeros((TILE, lanes), F32)
            for k in range(dm.top_k):
                hit = jnp.where(slot_of[c * KPAD + k:c * KPAD + k + 1] == srow, 1.0, hit)
            PG[pl.ds(r * TILE, TILE), pl.ds(c * lanes, lanes)] = hit.astype(BF16)

    def combine_rows(c):
        sl = SLT[c]
        gl = GLT[c]
        rows = pl.ds(c * crows, crows)
        for p in range(slots // KC):
            scol = (lax.broadcasted_iota(jnp.int32, (crows, KC), 1) + p * KC).astype(F32)
            w = jnp.zeros((crows, KC), F32)
            for k in range(dm.top_k):
                w = jnp.where(sl[:, k:k + 1] == scol, gl[:, k:k + 1], w)
            for i in range(3):
                part = w.astype(BF16)
                WC[rows, pl.ds(i * slots + p * KC, KC)] = part
                w = w - part.astype(F32)

    todo = [(2, j) for j in range(4, nj)] + [(3, j) for j in range(nj)]
    work = []
    for t in range(n):
        work.append(functools.partial(pick_rows, t))
        if t < nj - 6:
            work.append(functools.partial(shared_stage, t + 6))
        work.append(functools.partial(combine_rows, t))
    total = len(work)
    for u, (h, j) in enumerate(todo):
        forward(h, j)
        while len(work) > total * (len(todo) - 1 - u) // len(todo):
            work.pop(0)()
    for c in range(sff // KC):
        a = SACC[:, pl.ds(c * KC, KC)]
        g = SACC[:, pl.ds(sff + c * KC, KC)]
        HS[:, pl.ds(c * KC, KC)] = (jax.nn.silu(a) * g).astype(BF16)

    def last_hop(j, carry):
        forward(hops, j)
        return carry

    lax.fori_loop(0, nj, last_hop, 0)

    def arrive(j, carry):
        for h in range(1, hops + 1):
            x_d2d_in(j, h).wait_recv()
        return carry

    lax.fori_loop(0, nj, arrive, 0)
    for c in first:
        c.wait_send()
    for h in range(hops):
        blk = i_block(h, h + 1 == hops)
        rcopy(blk, blk, is_ring.at[h], ir_ring.at[h], down).wait_send()
        blk = i_block(h + 1, h + 1 == hops)
        rcopy(blk, blk, is_d2d.at[h], ir_d2d.at[h], partner).wait_send()

    def drain(j, carry):
        x_part(j, 0, False).wait_send()
        x_part(j, 0, True).wait_send()
        for h in range(hops):
            if h > 0:
                x_ring(j, h).wait_send()
            x_d2d(j, h + 1).wait_send()
        return carry

    lax.fori_loop(0, nj, drain, 0)


def up_kernel(dm, te_ref, x_ref, pg_ref, w1, w3, h_ref, xg_ref, w_ref, wsem):
    n_tiles = dm.slots // TILE
    nt = dm.ff // KC

    def copies(c, slot):
        cols = pl.ds(pl.multiple_of(c * KC, KC), KC)
        return [pltpu.make_async_copy(src.at[:, :, cols], w_ref.at[slot, m], wsem.at[slot, m]) for m, src in enumerate((w1, w3))]

    depth = w_ref.shape[0]
    for c in range(depth):
        start(copies(c, c))

    def pick(j, carry):
        xg_ref[:, pl.ds(pl.multiple_of(j * KC, KC), KC)] = dot(pg_ref[...], x_ref[j].reshape(pg_ref.shape[1], KC)).astype(BF16)
        return carry

    lax.fori_loop(0, dm.nj, pick, 0)

    def column(c, carry):
        slot = c % depth
        cols = pl.ds(pl.multiple_of(c * KC, KC), KC)
        wait(copies(c, slot))
        for i in range(n_tiles):
            rows = pl.ds(i * TILE, TILE)

            @pl.when(i < te_ref[n_tiles])
            def _():
                e = te_ref[i]
                a = dot(xg_ref[rows, :], w_ref[slot, 0, e])
                g = dot(xg_ref[rows, :], w_ref[slot, 1, e])
                h_ref[rows, cols] = (jax.nn.silu(a) * g).astype(BF16)

            @pl.when(i >= te_ref[n_tiles])
            def _():
                h_ref[rows, cols] = jnp.zeros((TILE, KC), BF16)

        @pl.when(c + depth < nt)
        def _():
            start(copies(c + depth, slot))
        return carry

    lax.fori_loop(0, nt, column, 0)


def down_kernel(dm, H, WC, TE, HS, resid_ref, ew2, sw2, out_ref,
                BIG, V2A, V2B, S2A, S2B, E3, PR, RR, FR, SOUT, vsem, qs, qr, rs, rr, fs, fr):
    n = dm.n_chip
    hops = n // 2
    tok = dm.tok
    crows = 2 * tok
    nj = dm.nj
    slots = dm.slots
    n_tiles = slots // TILE
    group = n * crows
    me, chip, core, at, partner, down, up = ring_place(dm)
    V2 = (V2A, V2B)
    S2 = (S2A, S2B)

    def down_copies(j, slot):
        cols = pl.ds(pl.multiple_of(j * KC, KC), KC)
        return [pltpu.make_async_copy(ew2.at[:, :, cols], V2[slot], vsem.at[slot, 0])]

    def shared_copies(j, slot):
        cols = pl.ds(pl.multiple_of(j * KC, KC), KC)
        return [pltpu.make_async_copy(sw2.at[:, cols], S2[slot], vsem.at[slot, 1])]

    def shared_step(j, slot, more):
        wait(shared_copies(j, slot))
        SOUT[j] = dot(HS[...], S2[slot][...]).astype(BF16)
        if more:
            start(shared_copies(j + 2, slot))

    start(down_copies(0, 0))
    start(down_copies(1, 1))
    entry_barrier((partner, down, up))

    pr_off = [448, 0, 128, 256, 384]
    assert crows == 128 and hops == 4

    def dblk(j, dest, row, size):
        return pl.ds(pl.multiple_of(j * group + dest * crows + row, tok), size)

    def q_copy(j, h):
        if h == 0:
            src, size = BIG.at[dblk(j, chip, (1 - core) * tok, tok), :], tok
        elif h == hops:
            src, size = BIG.at[dblk(j, at(-h), (1 - core) * tok, tok), :], tok
        else:
            src, size = BIG.at[dblk(j, at(-h), 0, crows), :], crows
        return rcopy(src, PR.at[j, pl.ds(pr_off[h], size), :], qs.at[h, j], qr.at[h, j], partner)

    rr_off = [0, 64, 192, 320]

    def r_copy(j, g):
        h = hops - g
        src, size = (BIG.at[dblk(j, at(h), core * tok, tok), :], tok) if g == 0 else (BIG.at[dblk(j, at(h), 0, crows), :], crows)
        return rcopy(src, RR.at[j, pl.ds(rr_off[g], size), :], rs.at[g, j], rr.at[g, j], down)

    def f_copy(j):
        return rcopy(RR.at[j, pl.ds(pl.multiple_of(rr_off[hops - 1] + (1 - core) * tok, tok), tok), :], FR.at[j], fs.at[j], fr.at[j], partner)

    def finish(j):
        q_copy(j, 0).wait_recv()
        f_copy(j).wait_recv()
        cols = pl.ds(pl.multiple_of(j * KC, KC), KC)
        routed = BIG[dblk(j, chip, core * tok, tok), :] + PR[j, pl.ds(pr_off[0], tok), :]
        routed = routed + RR[j, pl.ds(pl.multiple_of(rr_off[hops - 1] + core * tok, tok), tok), :] + FR[j]
        out_ref[:, cols] = (resid_ref[:, cols].astype(F32) + SOUT[j].astype(F32) + routed).astype(BF16)

    def turn(j):
        r_copy(j, hops - 1).wait_recv()
        f_copy(j).start()

    def relay(j, g):
        h = hops - g
        q_copy(j, h).wait_recv()
        if g == 0:
            rows = dblk(j, at(h), core * tok, tok)
            BIG[rows, :] += PR[j, pl.ds(pr_off[h], tok), :]
        else:
            r_copy(j, g - 1).wait_recv()
            rows = dblk(j, at(h), 0, crows)
            if g == 1:
                BIG[rows, :] += PR[j, pl.ds(pr_off[h], crows), :]
                hrows = dblk(j, at(h), core * tok, tok)
                BIG[hrows, :] += RR[j, pl.ds(rr_off[0], tok), :]
            else:
                BIG[rows, :] += PR[j, pl.ds(pr_off[h], crows), :] + RR[j, pl.ds(rr_off[g - 1], crows), :]
        r_copy(j, g).start()

    skew = 2
    late = nj // 2

    def ring(s, static):
        def ok(j):
            return (0 <= j < nj) if static else (j >= 0)
        for g in range(hops):
            j = s - skew * (g + 1)
            cond(static, ok(j), functools.partial(relay, j, g))
        j = s - skew * (hops + 1)
        cond(static, ok(j), functools.partial(turn, j))
        cond(static, ok(j - 1), functools.partial(finish, j - 1))

    def down_step(j, slot):
        ring(j, False)
        wait(down_copies(j, slot))
        for i in range(n_tiles):
            e = dot(H[pl.ds(i * TILE, TILE), :], V2[slot][TE[i]]).astype(BF16)
            for p in range(3):
                E3[pl.ds(p * slots + i * TILE, TILE), :] = e
        for r in range(group // KC):
            rows = pl.ds(pl.multiple_of(j * group + r * KC, KC), KC)
            BIG[rows, :] = dot(WC[pl.ds(r * KC, KC), :], E3[...])
        for h in range(hops, -1, -1):
            q_copy(j, h).start()

        @pl.when(j + 2 < nj)
        def _():
            start(down_copies(j + 2, slot))

        @pl.when(j == 0)
        def _():
            start(shared_copies(0, 0))
            start(shared_copies(1, 1))

        @pl.when(j >= late)
        def _():
            shared_step(j - late, (slot + late) % 2, True)

    def down_pair(p, carry):
        for q in range(2):
            down_step(2 * p + q, q)
        return carry

    lax.fori_loop(0, nj // 2, down_pair, 0)
    for s in range(nj, nj + skew * (hops + 1) + 1):
        ring(s, True)
        if 0 <= s - late < nj:
            shared_step(s - late, (s - late) % 2, s - late + 2 < nj)

    def drain(j, carry):
        for h in range(hops):
            r_copy(j, h).wait_send()
        for h in range(hops + 1):
            q_copy(j, h).wait_send()
        f_copy(j).wait_send()
        return carry

    lax.fori_loop(0, nj, drain, 0)


class Dims:
    pass


def solution(mesh):
    n_ep = mesh.shape['ep']
    tok_spec = P(('dp', 'ep'))
    expert_spec = P('ep')

    def device_fn(resid_in, expert_ids, priority, norm_gain, router_w, shared_w1, shared_w3, shared_w2, expert_w1, expert_w3, expert_w2):
        dm = Dims()
        dm.n_chip = n_ep // 2
        dm.tok, dm.hidden = resid_in.shape
        dm.top_k = expert_ids.shape[1]
        dm.local_e = expert_w1.shape[0]
        dm.ff = expert_w1.shape[2]
        dm.capacity = dm.tok * dm.top_k
        dm.nj = dm.hidden // KC
        dm.sff = shared_w1.shape[1]
        dm.slots = (dm.capacity + dm.local_e * (TILE - 1)) // TILE * TILE
        hops = dm.n_chip // 2
        assert dm.nj % 2 == 0
        nj, tok, ff, slots = dm.nj, dm.tok, dm.ff, dm.slots
        group = dm.n_chip * 2 * tok

        vm = pl.BlockSpec(memory_space=pltpu.VMEM)
        sm = pl.BlockSpec(memory_space=pltpu.SMEM)
        hbm = pl.BlockSpec(memory_space=pltpu.HBM)
        dma = pltpu.SemaphoreType.DMA
        le = dm.local_e
        rows_in = jnp.concatenate([resid_in, router_w.T], axis=0)

        n_small = 1 + 2 * dm.top_k

        def wide(a, first):
            return lax.pad(a.T, jnp.int32(0), ((first, n_small - first - dm.top_k, 0), (0, dm.hidden - tok, 0)))

        gain_rows = lax.broadcast_in_dim(norm_gain, (n_small, dm.hidden), (1,))
        is_gain = lax.broadcasted_iota(jnp.int32, (n_small, dm.hidden), 0) == 0
        small_in = jnp.where(is_gain, gain_rows, (wide(expert_ids, 1) + wide(priority, 1 + dm.top_k)).astype(F32))
        rows_all, pick_rows, mix, shared_act, tile_e = pl.pallas_call(
            functools.partial(gather_kernel, dm),
            out_shape=(jax.ShapeDtypeStruct((nj, dm.n_chip, 2 * tok, KC), BF16), jax.ShapeDtypeStruct((slots, group), BF16),
                       jax.ShapeDtypeStruct((group, 3 * slots), BF16), jax.ShapeDtypeStruct((tok, dm.sff), BF16),
                       jax.ShapeDtypeStruct((slots // TILE + 1,), jnp.int32)),
            in_specs=[vm, vm, hbm, hbm],
            out_specs=(vm, vm, vm, vm, sm),
            scratch_shapes=[
                pltpu.VMEM((nj, tok, KC), BF16),
                pltpu.VMEM((dm.n_chip, 2, 3 * KPAD, 2 * tok), F32),
                pltpu.VMEM((dm.n_chip, 2 * tok, KPAD), F32),
                pltpu.VMEM((dm.n_chip, 2 * tok, KPAD), F32),
                pltpu.VMEM((tok, 2 * dm.sff), F32),
                pltpu.VMEM((2, 2, KC, dm.sff), BF16),
                dma((2, 2)), dma((nj,)), dma((nj,)),
                dma((hops, nj)), dma((hops, nj)), dma((hops, nj)), dma((hops, nj)),
                dma((hops,)), dma((hops,)), dma((hops,)), dma((hops,)), dma((2,)), dma((2,)),
            ],
            compiler_params=pltpu.CompilerParams(collective_id=0, has_side_effects=True, vmem_limit_bytes=36 << 20),
        )(rows_in, small_in, shared_w1, shared_w3)
        h_act = pl.pallas_call(
            functools.partial(up_kernel, dm),
            out_shape=jax.ShapeDtypeStruct((slots, ff), BF16),
            in_specs=[sm, vm, vm, hbm, hbm],
            out_specs=vm,
            scratch_shapes=[pltpu.VMEM((slots, dm.hidden), BF16), pltpu.VMEM((3, 2, le, dm.hidden, KC), BF16), dma((3, 2))],
            compiler_params=pltpu.CompilerParams(vmem_limit_bytes=40 << 20),
        )(tile_e, rows_all, pick_rows, expert_w1, expert_w3)
        return pl.pallas_call(
            functools.partial(down_kernel, dm),
            out_shape=jax.ShapeDtypeStruct((tok, dm.hidden), BF16),
            in_specs=[vm, vm, sm, vm, vm, hbm, hbm],
            out_specs=vm,
            scratch_shapes=[
                pltpu.VMEM((nj * group, KC), F32),
                pltpu.VMEM((le, ff, KC), BF16),
                pltpu.VMEM((le, ff, KC), BF16),
                pltpu.VMEM((dm.sff, KC), BF16),
                pltpu.VMEM((dm.sff, KC), BF16),
                pltpu.VMEM((3 * slots, KC), BF16),
                pltpu.VMEM((nj, 8 * tok, KC), F32),
                pltpu.VMEM((nj, 7 * tok, KC), F32),
                pltpu.VMEM((nj, tok, KC), F32),
                pltpu.VMEM((nj, tok, KC), BF16),
                dma((2, 2)),
                dma((hops + 1, nj)), dma((hops + 1, nj)), dma((hops, nj)), dma((hops, nj)), dma((nj,)), dma((nj,)),
            ],
            compiler_params=pltpu.CompilerParams(collective_id=1, has_side_effects=True, vmem_limit_bytes=38 << 20),
        )(h_act, mix, tile_e, shared_act, resid_in, expert_w2, shared_w2)

    return jax.shard_map(device_fn, mesh=mesh, in_specs=(tok_spec, tok_spec, tok_spec, P(), P(), P(), P(), P(), expert_spec, expert_spec, expert_spec), out_specs=tok_spec, check_vma=False)
```
